128 devices in a mesh: cells: 16 (over y, x), mem: 8 (over z, core).
Axes of the slice: x: 4, y: 4, z: 4, core: 2. Of those that a mesh axis runs over, the one named last changes fastest.
Arguments:
- background_realisations: bfloat16 [128, 4096, 128], P('mem', 'cells'), may hold values from -6 to 6
- reading_figures: float32 [4096, 128], P('cells'), may hold values from -6 to 6
- reading_error_spread: float32 [4096, 128], P('cells'), may hold values from 0.5 to 4
- footprint_grid_point: int32 [4096, 128], P('cells'), may hold values from 0 to 31
- active_reading_number: int32 [4096], P('cells'), may hold values from 0 to 128, as said below
- bordering_patches: int32 [4096, 4], P('cells'), may hold values from 0 to 4095, as said below
Outputs:
- analysis: bfloat16 [128, 4096, 128], P('mem', 'cells')
The draws below stay inside these ranges and needn't reach their ends.
Inputs may be any that keep to these rules, and one draw needn't show every extreme that they name: The live observations of tile t fill its first active_reading_number[t] slots; in every draw some tile has all 128 slots live; counts differ strongly between runs of 32 tiles. `bordering_patches`: each row lists 4 different tiles, never the row's own tile, each at circular distance 1 to 128 from it along the order of the 4096 tiles.
All inputs are finite; a program needn't handle non-finite values.
Results may differ from the reference program's by a relative error of at most 0.01.
Values may be sent and summed in bfloat16 or wider, within the bound.
No kernel may reach another device: no remote copies, remote signals or barrier semaphores. Data moves between devices by JAX's collectives and lax.ppermute only.
A program may use at most 128 MiB of HBM per device.

```python
import math
import jax
import jax.numpy as jnp
from jax import lax

RUN_NUMBER = 128
GRID_POINTS_EACH = 32
VECTOR_SPAN = 128
OBS_SLOTS = 128
TILES_DEV = 256
NEIGHBORS = 4
RADIUS = 128
SWEEPS = 6
PATCH_NUMBER = 4096
N_MEM = 8


def draw_active_reading_number(key, part):
    level_key = jax.random.fold_in(key, 11)
    count_key = jax.random.fold_in(key, 12)
    full_key = jax.random.fold_in(key, 13)
    region = jnp.arange(PATCH_NUMBER) // 32
    levels = jax.random.randint(level_key, (PATCH_NUMBER // 32 + 1,), 2, 5)
    ceiling = levels[region] * OBS_SLOTS // 4
    floor_part = ceiling // 4
    counts = floor_part + jax.random.randint(count_key, (PATCH_NUMBER,), 0, ceiling - floor_part + 1)
    full_tile = jax.random.randint(full_key, (), 0, PATCH_NUMBER)
    return jnp.where(jnp.arange(PATCH_NUMBER) == full_tile, OBS_SLOTS, counts).astype(jnp.int32)


def draw_bordering_patches(key, part):
    candidates = 2 * RADIUS
    scores = jax.random.randint(jax.random.fold_in(key, 21), (PATCH_NUMBER, candidates), 0, 1 << 20) * candidates + jnp.arange(candidates)
    chosen = jnp.argsort(scores, axis=1)[:, :NEIGHBORS]
    offsets = jnp.where(chosen < RADIUS, chosen - RADIUS, chosen - RADIUS + 1)
    return ((jnp.arange(PATCH_NUMBER)[:, None] + offsets) % PATCH_NUMBER).astype(jnp.int32)


def set_ends(drawn, rng, smallest, high):
    longest = drawn.shape.index(max(drawn.shape))
    spots = []
    for shift in (0, 1):
        where = [jax.random.randint(jax.random.fold_in(rng, axis), (), 0, length) for axis, length in enumerate(drawn.shape)]
        where[longest] = (where[longest] + shift) % drawn.shape[longest]
        spots.append(tuple(where))
    return drawn.at[spots[0]].set(smallest).at[spots[1]].set(high)


def block_levels(stream_key, extent, split, smallest, top_value):
    level = 1.0
    for axis_at, blocks in split:
        heights = jax.random.uniform(jax.random.fold_in(jax.random.fold_in(stream_key, 6), axis_at), (blocks,), jnp.float32, smallest / len(split), top_value / len(split))
        level = level * jnp.repeat(jnp.exp(heights), extent[axis_at] // blocks).reshape((-1,) + (1,) * (len(extent) - 1 - axis_at))
    return level


def normal_values(stream_key, shape, scale, most, cuts=(), held_as=jnp.bfloat16):
    factor_of = block_levels(stream_key, shape, cuts, -0.22, 0.18) if cuts else 1.0
    entries = jax.random.normal(stream_key, shape, jnp.float32) * scale * factor_of
    return jnp.minimum(jnp.maximum(entries, -most), most).astype(held_as)


def setup_inputs(seed: int = 0) -> dict:
    streams_of = jax.random.split(jax.random.key(seed), 7)
    return {
        "background_realisations": normal_values(streams_of[0], (RUN_NUMBER, PATCH_NUMBER, VECTOR_SPAN), 1.0, 6.0, ((0, 8), (1, 16))),
        "reading_figures": normal_values(streams_of[1], (PATCH_NUMBER, OBS_SLOTS), 1.0, 6.0, ((0, 16),), jnp.float32),
        "reading_error_spread": jnp.clip(jnp.exp(math.log(4.0) - 2.0794415 * jax.random.uniform(streams_of[2], (PATCH_NUMBER, OBS_SLOTS), jnp.float32) ** block_levels(streams_of[2], (PATCH_NUMBER, OBS_SLOTS), ((0, 16),), -0.2, 0.2)), 0.5, 4.0),
        "footprint_grid_point": set_ends(jax.random.randint(streams_of[3], (PATCH_NUMBER, OBS_SLOTS), 0, GRID_POINTS_EACH), jax.random.fold_in(streams_of[3], 1), 0, GRID_POINTS_EACH - 1).astype(jnp.int32),
        "active_reading_number": draw_active_reading_number(jax.random.fold_in(streams_of[6], 71), 0),
        "bordering_patches": draw_bordering_patches(jax.random.fold_in(streams_of[6], 71), 0),
    }


def batched(left, right):
    return jnp.einsum('bij,bjk->bik', left, right, precision=lax.Precision.HIGHEST)

def inverse_root(system, sweeps):
    norm_scale = jnp.sqrt(lax.optimization_barrier(jnp.sum(system * system, axis=(1, 2))))
    identity = jnp.eye(system.shape[1], dtype=jnp.float32)[None]
    other_iter = system / norm_scale[:, None, None]
    root_iter = jnp.broadcast_to(identity, system.shape)
    for sweep_index in range(sweeps):
        step_matrix = 1.5 * identity - 0.5 * batched(root_iter, other_iter)
        other_iter = batched(other_iter, step_matrix)
        root_iter = batched(step_matrix, root_iter)
    return (root_iter, norm_scale)

def make_transform(gram_sum, cross_sum, members):
    identity = jnp.eye(members, dtype=jnp.float32)[None]
    system = (members - 1.0) * identity + gram_sum
    root_iter, norm_scale = inverse_root(system, SWEEPS)
    spread = jnp.sqrt((members - 1.0) / norm_scale)[:, None, None] * root_iter
    inner = jnp.einsum('bij,bj->bi', root_iter, cross_sum, precision=lax.Precision.HIGHEST)
    mean_weight = jnp.einsum('bij,bj->bi', root_iter, inner, precision=lax.Precision.HIGHEST) / norm_scale[:, None]
    return (spread + mean_weight[:, :, None]).astype(jnp.bfloat16)

def reference(background_realisations, reading_figures, reading_error_spread, footprint_grid_point, active_reading_number, bordering_patches):
    background_centroid = lax.optimization_barrier(jnp.mean(background_realisations.astype(jnp.float32), axis=0))
    realisation_offset_from_centroid = (background_realisations.astype(jnp.float32) - background_centroid).astype(jnp.bfloat16)
    sensed_readings = background_realisations[:, :, :GRID_POINTS_EACH].astype(jnp.float32) + 0.5 * background_realisations[:, :, GRID_POINTS_EACH:2 * GRID_POINTS_EACH].astype(jnp.float32)
    picked_obs = jnp.take_along_axis(sensed_readings, footprint_grid_point[None].astype(jnp.int32), axis=2)
    live = jnp.arange(OBS_SLOTS, dtype=jnp.int32)[None, :] < active_reading_number[:, None]
    weight = jnp.where(live, 1.0 / jnp.sqrt(reading_error_spread), 0.0).astype(jnp.float32)
    scaled = (weight[None] * picked_obs).astype(jnp.bfloat16)
    scaled_mean = lax.optimization_barrier(jnp.mean(scaled.astype(jnp.float32), axis=0))
    obs_anomaly = (scaled.astype(jnp.float32) - scaled_mean).astype(jnp.bfloat16)
    innovation = (weight * reading_figures - scaled_mean).astype(jnp.bfloat16)
    stacked = jnp.concatenate([obs_anomaly, innovation[None]], axis=0)
    tile_ids = jnp.arange(PATCH_NUMBER, dtype=jnp.int32)
    tile_list = jnp.concatenate([tile_ids[:, None], bordering_patches.astype(jnp.int32)], axis=1)
    forward_gap = (tile_list - tile_ids[:, None]) % PATCH_NUMBER
    distance = jnp.minimum(forward_gap, PATCH_NUMBER - forward_gap)
    taper_weight = 1.0 - distance.astype(jnp.float32) / (RADIUS + 1.0)
    group_of_blocks = TILES_DEV // N_MEM
    count = PATCH_NUMBER // group_of_blocks

    def solve_batch(leading_line):
        own_list = lax.dynamic_slice_in_dim(tile_list, leading_line, group_of_blocks, 0)
        own_taper = lax.dynamic_slice_in_dim(taper_weight, leading_line, group_of_blocks, 0)
        gram_sum = jnp.zeros((group_of_blocks, RUN_NUMBER, RUN_NUMBER), jnp.float32)
        cross_sum = jnp.zeros((group_of_blocks, RUN_NUMBER), jnp.float32)
        for entry in range(NEIGHBORS + 1):
            picked = jnp.take(stacked, own_list[:, entry], axis=1).astype(jnp.float32)
            pick_anomaly = picked[:RUN_NUMBER]
            pick_innov = picked[RUN_NUMBER]
            gram_sum = gram_sum + own_taper[:, entry, None, None] * jnp.einsum('kbo,lbo->bkl', pick_anomaly, pick_anomaly, precision=lax.Precision.HIGHEST)
            cross_sum = cross_sum + own_taper[:, entry, None] * jnp.einsum('kbo,bo->bk', pick_anomaly, pick_innov, precision=lax.Precision.HIGHEST)
        transform = make_transform(gram_sum, cross_sum, RUN_NUMBER)
        own_anomaly = lax.dynamic_slice_in_dim(realisation_offset_from_centroid, leading_line, group_of_blocks, 1).astype(jnp.float32)
        self_centroid = lax.dynamic_slice_in_dim(background_centroid, leading_line, group_of_blocks, 0)
        posterior_realisations = jnp.einsum('ibs,bim->mbs', own_anomaly, transform.astype(jnp.float32), precision=lax.Precision.HIGHEST)
        return (posterior_realisations + self_centroid[None]).astype(jnp.bfloat16)
    pieces = lax.map(solve_batch, jnp.arange(count, dtype=jnp.int32) * group_of_blocks)
    return jnp.moveaxis(pieces, 0, 1).reshape(RUN_NUMBER, PATCH_NUMBER, VECTOR_SPAN)
```

```python
import jax
import jax.numpy as jnp
from jax import lax
from jax.experimental import pallas as pl
from jax.experimental.pallas import tpu as pltpu
from jax.sharding import Mesh
from jax.sharding import PartitionSpec as P

F32 = jnp.float32
BF16 = jnp.bfloat16
MEM = ("z", "k")
PACK = 4
UNROLL = 4


def lane_id(rows):
    return lax.broadcasted_iota(jnp.int32, (rows, 128), 1)


def sense_kernel(bg, xt, sg, buf):
    members, tiles, _ = bg.shape
    for m in range(members):
        buf[pl.ds(m, tiles, stride=members), :] = bg[m].astype(F32)
    quarter = lane_id(members) >> 5

    def group(g, carry):
        row = None
        for q in range(PACK):
            at = pl.multiple_of((PACK * g + q) * members, members)
            x = buf[pl.ds(at, members), :]
            xt[PACK * g + q] = x.astype(BF16)
            s = x + 0.5 * pltpu.roll(x, 96, 1)
            s = s if q == 0 else pltpu.roll(s, 32 * q, 1)
            row = s if q == 0 else jnp.where(quarter == q, s, row)
        sg[g] = row.astype(BF16)
        return carry

    lax.fori_loop(0, tiles // PACK, group, 0, unroll=4)


def cell_kernel(pix, w2, y, out):
    groups = pix.shape[0] // PACK

    def packed(ref, p):
        parts = [ref[pl.ds(2 * p + h, groups, stride=PACK), :] for h in range(2)]
        return jnp.concatenate(parts, axis=0).astype(F32).T

    cols = [[], []]
    for p in range(2):
        pt = packed(pix, p)
        wt = packed(w2, p)
        yt = packed(y, p) * wt
        d, e = [], []
        for c in range(32):
            hit = pt == float(c)
            d.append(jnp.sum(jnp.where(hit, wt, 0.0), axis=0, keepdims=True))
            e.append(jnp.sum(jnp.where(hit, yt, 0.0), axis=0, keepdims=True))
        for i, rows in enumerate((d, e)):
            block = jnp.concatenate(rows, axis=0)
            cols[i] += [block, pltpu.roll(block, 64, 1)]
    for i in range(2):
        out[i] = jnp.concatenate(cols[i], axis=0).T[:groups]


def split(a):
    hi = a.astype(BF16)
    return hi, (a - hi.astype(F32)).astype(BF16)


def mul(left, right):
    lhs = jnp.concatenate(left, axis=1)
    half = jnp.concatenate(right, axis=1)
    both = jnp.dot(lhs, jnp.concatenate([half, half], axis=0), preferred_element_type=F32)
    return both[:, :128] + both[:, 128:]


def each(f, *lists):
    return [f(*a) for a in zip(*lists)]


def solve_kernel(info, nbr, ext, r1, r2, r3, extp, p1, p2, p3, de, out, G, E):
    z, k, first, total = info[0], info[1], info[2], info[3]
    reach = 128
    base = 16 * z + 8 * k

    def center(g, carry):
        b0 = base + g
        b = 8 * k + g
        parts = [ext[b0], r1[b], r2[b], r3[b], extp[b0], p1[b], p2[b], p3[b]]
        x = jnp.concatenate(parts, axis=0).astype(F32)
        mean = jnp.sum(x, axis=0, keepdims=True) * (1.0 / 128.0)
        G[g] = (x - mean).astype(BF16)
        E[pl.ds(g, 1), :] = de[1, pl.ds(b0, 1), :] - de[0, pl.ds(b0, 1), :] * mean
        return carry

    lax.fori_loop(0, G.shape[0], center, 0, unroll=4)
    quarter = lane_id(1) >> 5
    eye = lax.broadcasted_iota(jnp.int32, (128, 128), 0) == lane_id(128)

    def gather(t):
        lhs, rhs, inn = [], [], []
        for n in range(5):
            if n == 0:
                loc, tap = t + reach, 1.0
            else:
                gap = nbr[t, n - 1] - (first + t)
                gap = jnp.where(gap < 0, gap + total, gap)
                gap = jnp.where(gap > total // 2, gap - total, gap)
                loc = t + reach + gap
                tap = 1.0 - jnp.abs(gap).astype(F32) * (1.0 / (reach + 1.0))
            g = loc // PACK
            mask = jnp.where(quarter == loc % PACK, tap, 0.0)
            block = G[g]
            drow = de[0, pl.ds(base + g, 1), :] * mask
            erow = E[pl.ds(g, 1), :] * mask
            lhs.append(block * drow.astype(BF16))
            rhs.append(block)
            inn.append(jnp.broadcast_to(erow, (16, 128)).astype(BF16))
        left = jnp.concatenate([jnp.concatenate(lhs, axis=1), jnp.concatenate(inn, axis=1)], axis=0)
        right = jnp.concatenate(rhs, axis=1)
        return lax.dot_general(left, right, (((1,), (1,)), ((), ())), preferred_element_type=F32)

    def tiles(b, carry):
        ts = [b * UNROLL + u for u in range(UNROLL)]
        both = [gather(t) for t in ts]
        system = [a[:128] + jnp.where(eye, 127.0, 0.0) for a in both]
        cross = [a[128:129] for a in both]
        inv = [
            lax.rsqrt(jnp.sum(jnp.sum(a * a, axis=0, keepdims=True), axis=1, keepdims=True))
            for a in system
        ]
        w = each(lambda a, i: a * i, system, inv)
        root = None
        for step in range(3):
            ws = each(split, w)
            w2 = each(mul, ws, ws)
            w2s = each(split, w2)
            tail = each(lambda a, c: split(-0.5625 * a + 0.0625 * c), w, w2)
            high = each(mul, w2s, tail)
            q = each(
                lambda a, c, h: jnp.where(eye, 2.25, 0.0) - 2.4375 * a + 1.6875 * c + h, w, w2, high
            )
            qs = each(split, q)
            root = q if root is None else each(lambda a, r: mul(a, split(r)), qs, root)
            if step < 2:
                half = each(mul, ws, qs)
                w = each(lambda a, c: mul(split(a), c), half, qs)
        for u, t in enumerate(ts):
            r = root[u]
            col = jnp.sum(r * cross[u], axis=1, keepdims=True)
            row = jnp.sum(r * col, axis=0, keepdims=True) * inv[u]
            out[t] = (r * jnp.sqrt(127.0 * inv[u]) + row).astype(BF16)
        return carry

    lax.fori_loop(0, out.shape[0] // UNROLL, tiles, 0)


def update_kernel(info, tr, xt, s1, s2, s3, q0, q1, q2, q3, *outs):
    z, k = info[0], info[1]

    def tile(t, carry):
        b = 32 * k + t
        parts = [xt[64 * z + b], s1[b], s2[b], s3[b], q0[b], q1[b], q2[b], q3[b]]
        x = jnp.concatenate(parts, axis=0).astype(F32)
        mean = jnp.sum(x, axis=0, keepdims=True) * (1.0 / 128.0)
        anomaly = (x - mean).astype(BF16)
        new = jnp.dot(tr[t], anomaly, preferred_element_type=F32) + mean
        new = new.astype(BF16)
        for i, o in enumerate(outs):
            o[t] = new[16 * i : 16 * i + 16]
        return carry

    lax.fori_loop(0, tr.shape[0], tile, 0, unroll=4)


def place_kernel(info, *refs):
    pieces, out, buf = refs[:8], refs[8], refs[9]
    z, k = info[0], info[1]
    for i, piece in enumerate(pieces):
        d, o = i % 4, i // 4
        zz = (z + d) % 4
        kk = k if o == 0 else 1 - k
        at = pl.multiple_of(64 * zz + 32 * kk, 32)
        for t in range(32):
            buf[pl.ds(t, 16, stride=32), :] = piece[t].astype(F32)
        for m in range(16):
            out[m, pl.ds(at, 32), :] = buf[32 * m : 32 * m + 32, :].astype(BF16)


def vmem():
    return pl.BlockSpec(memory_space=pltpu.VMEM)


def smem():
    return pl.BlockSpec(memory_space=pltpu.SMEM)


def call(kernel, n_smem, args, outs, scratch=()):
    return pl.pallas_call(
        kernel,
        in_specs=[smem()] * n_smem + [vmem()] * (len(args) - n_smem),
        out_specs=jax.tree.map(lambda _: vmem(), outs),
        out_shape=outs,
        scratch_shapes=list(scratch),
        compiler_params=pltpu.CompilerParams(vmem_limit_bytes=48 * 1024 * 1024),
    )(*args)


def to_z(x, by):
    return lax.ppermute(x, "z", [(i, (i + by) % 4) for i in range(4)])


def to_core(x):
    return lax.ppermute(x, "k", [(0, 1), (1, 0)])


def to_cells(x, by):
    n = lax.axis_size("cells")
    return lax.ppermute(x, "cells", [(i, (i + by) % n) for i in range(n)])


def home(x, d, o):
    pairs = [(2 * z + k, 2 * ((z - d) % 4) + (k ^ o)) for z in range(4) for k in range(2)]
    return lax.ppermute(x, MEM, pairs)


def per_device(bg, figures, spread, pixel, active, nbr):
    members, tiles, width = bg.shape
    groups = tiles // PACK
    z, k = lax.axis_index("z"), lax.axis_index("k")
    first = lax.axis_index("cells") * tiles + 64 * z + 32 * k
    info = jnp.stack([z, k, first, tiles * lax.axis_size("cells")]).astype(jnp.int32)
    xt, sg = call(
        sense_kernel,
        0,
        (bg,),
        (
            jax.ShapeDtypeStruct((tiles, members, width), BF16),
            jax.ShapeDtypeStruct((groups, members, width), BF16),
        ),
        [pltpu.VMEM((tiles * members, width), F32)],
    )
    half = groups // 2
    ext = jnp.concatenate([to_cells(sg[half:], 1), sg, to_cells(sg[:half], -1)], axis=0)

    live = jnp.arange(128, dtype=jnp.int32)[None, :] < active[:, None]
    w2 = jnp.where(live, 1.0 / spread, 0.0)
    de = call(
        cell_kernel, 0, (pixel, w2, figures), jax.ShapeDtypeStruct((2, groups, 128), F32)
    )
    de = jnp.concatenate([to_cells(de[:, half:], 1), de, to_cells(de[:, :half], -1)], axis=1)

    got = []
    for d in (1, 2, 3):
        window = lax.dynamic_slice_in_dim(ext, ((z + d) % 4) * 16, 80, 0)
        got.append(to_z(window, d))
    extp = to_core(ext)
    gotp = [to_core(r) for r in got]
    own_nbr = lax.dynamic_slice_in_dim(nbr, 64 * z + 32 * k, 32, 0)
    transform = call(
        solve_kernel,
        2,
        (info, own_nbr, ext, *got, extp, *gotp, de),
        jax.ShapeDtypeStruct((32, 128, 128), BF16),
        [pltpu.VMEM((72, 128, 128), BF16), pltpu.VMEM((72, 128), F32)],
    )
    xs, _ = lax.optimization_barrier((xt, got[-1][:1]))
    part = []
    for d in (1, 2, 3):
        part.append(to_z(lax.dynamic_slice_in_dim(xs, ((z + d) % 4) * 64, 64, 0), d))
    partp = [to_core(lax.dynamic_slice_in_dim(xs, z * 64, 64, 0))] + [to_core(s) for s in part]
    piece = jax.ShapeDtypeStruct((32, members, width), BF16)
    outs = call(update_kernel, 1, (info, transform, xs, *part, *partp), (piece,) * 8)
    back = [
        outs[i] if i == 0 else home(outs[i], i % 4, i // 4) for i in range(8)
    ]
    return call(
        place_kernel,
        1,
        (info, *back),
        jax.ShapeDtypeStruct((members, tiles, width), BF16),
        [pltpu.VMEM((512, 128), F32)],
    )


def solution(mesh):
    finer = Mesh(mesh.devices.reshape(mesh.shape["cells"], 4, 2), ("cells", "z", "k"))
    placed = (
        P(MEM, "cells", None),
        P("cells", None),
        P("cells", None),
        P("cells", None),
        P("cells"),
        P("cells", None),
    )
    return jax.shard_map(
        per_device, mesh=finer, in_specs=placed, out_specs=P(MEM, "cells", None), check_vma=False
    )
```

```python
import jax
import jax.numpy as jnp
from jax import lax
from jax.experimental import pallas as pl
from jax.experimental.pallas import tpu as pltpu
from jax.sharding import Mesh
from jax.sharding import PartitionSpec as P

F32 = jnp.float32
BF16 = jnp.bfloat16
MEM = ("z", "k")
PACK = 4
UNROLL = 16


def lane_id(rows):
    return lax.broadcasted_iota(jnp.int32, (rows, 128), 1)


def sense_kernel(info, bg, sg, h0, h1, h2, h3, x0, x1, x2, x3, buf):
    members, tiles, _ = bg.shape
    z = info[0]
    pitch = tiles + 1
    for m in range(members):
        buf[pl.ds(m * pitch, tiles), :] = bg[m].astype(F32)
    quarter = lane_id(members) >> 5
    chunk = tiles // 4
    for d, xd in enumerate((x0, x1, x2, x3)):
        zone = (z + d) % 4

        def group(i, carry, xd=xd, zone=zone):
            row = None
            for q in range(PACK):
                x = buf[pl.ds(chunk * zone + PACK * i + q, members, stride=pitch), :]
                xd[PACK * i + q] = x.astype(BF16)
                s = x + 0.5 * pltpu.roll(x, 96, 1)
                s = s if q == 0 else pltpu.roll(s, 32 * q, 1)
                row = s if q == 0 else jnp.where(quarter == q, s, row)
            sg[(chunk // PACK) * zone + i] = row.astype(BF16)
            return carry

        lax.fori_loop(0, chunk // PACK, group, 0, unroll=8)
    for d, h in enumerate((h0, h1, h2, h3)):
        at = jnp.where((z + d) % 4 < 2, 32, 0)
        for i in range(32):
            h[i] = sg[at + i]


def cell_kernel(info, pix, w2, y, out, near):
    groups = pix.shape[0] // PACK

    def packed(ref, p):
        parts = [ref[pl.ds(2 * p + h, groups, stride=PACK), :] for h in range(2)]
        return jnp.concatenate(parts, axis=0).astype(F32).T

    cols = [[], []]
    for p in range(2):
        pt = packed(pix, p)
        wt = packed(w2, p)
        yt = packed(y, p) * wt
        d, e = [], []
        for c in range(32):
            hit = pt == float(c)
            d.append(jnp.sum(jnp.where(hit, wt, 0.0), axis=0, keepdims=True))
            e.append(jnp.sum(jnp.where(hit, yt, 0.0), axis=0, keepdims=True))
        for i, rows in enumerate((d, e)):
            block = jnp.concatenate(rows, axis=0)
            cols[i] += [block, pltpu.roll(block, 64, 1)]
    at = pl.multiple_of(jnp.where(info[0] < 2, 32, 0), 32)
    for i in range(2):
        out[i] = jnp.concatenate(cols[i], axis=0).T[:groups]
        near[i] = out[i, pl.ds(at, 32), :]


def split(a):
    hi = a.astype(BF16)
    return hi, (a - hi.astype(F32)).astype(BF16)


def mul(left, right):
    lhs = jnp.concatenate(left, axis=1)
    half = jnp.concatenate(right, axis=1)
    both = jnp.dot(lhs, jnp.concatenate([half, half], axis=0), preferred_element_type=F32)
    return both[:, :128] + both[:, 128:]


def each(f, *lists):
    return [f(*a) for a in zip(*lists)]


def solve_kernel(info, nbr, *refs):
    own, ends, (de, dn, out, gt, lt, et) = refs[:8], refs[8:16], refs[16:]
    z, k, first, total = info[0], info[1], info[2], info[3]
    reach = 128
    start = 16 * z - 32 + 8 * k
    low = z < 2
    n_end = jnp.where(low, -start, start + 8)
    end_at = jnp.where(low, 32 + start, 0)
    end_to = jnp.where(low, 0, 64 - start)
    own_at = jnp.where(low, 0, start)
    own_to = jnp.where(low, -start, 0)

    def center(src, table, b, g):
        x = jnp.concatenate([r[b] for r in src], axis=0).astype(F32)
        mean = jnp.sum(x, axis=0, keepdims=True) * (1.0 / 128.0)
        d = table[0, pl.ds(b, 1), :]
        e = table[1, pl.ds(b, 1), :] - d * mean
        a = x - mean
        gt[g] = a.astype(BF16).T
        lt[g] = (a * d).astype(BF16).T
        et[g] = jnp.broadcast_to(e, (8, 128)).T.astype(BF16)

    def own_eight(j, carry):
        for i in range(8):
            center(own, de, own_at + 8 * j + i, own_to + 8 * j + i)
        return carry

    def end_eight(j, carry):
        for i in range(8):
            center(ends, dn, end_at + 8 * j + i, end_to + 8 * j + i)
        return carry

    lax.fori_loop(0, (gt.shape[0] - n_end) // 8, own_eight, 0)
    lax.fori_loop(0, n_end // 8, end_eight, 0)
    eye = lax.broadcasted_iota(jnp.int32, (128, 128), 0) == lane_id(128)

    def gather(t):
        lhs, extra, rhs = [], [], []
        for n in range(5):
            if n == 0:
                loc, tap = t + reach, None
            else:
                gap = nbr[t, n - 1] - (first + t)
                gap = jnp.where(gap < 0, gap + total, gap)
                gap = jnp.where(gap > total // 2, gap - total, gap)
                loc = t + reach + gap
                tap = (1.0 - jnp.abs(gap).astype(F32) * (1.0 / (reach + 1.0)))
            g = loc // PACK
            at = pl.multiple_of(32 * (loc % PACK), 32)
            rhs.append(gt[g, pl.ds(at, 32), :])
            for store, ref in ((lhs, lt), (extra, et)):
                v = ref[g, pl.ds(at, 32), :]
                store.append(v if tap is None else (v.astype(F32) * tap).astype(BF16))
        cat = lambda v: jnp.concatenate(v, axis=0)
        right = cat(rhs)
        dims = (((0,), (0,)), ((), ()))
        gram = lax.dot_general(cat(lhs), right, dims, preferred_element_type=F32)
        cross = lax.dot_general(cat(extra), right, dims, preferred_element_type=F32)
        return gram, cross

    def tiles(b, carry):
        ts = [b * UNROLL + u for u in range(UNROLL)]
        both = [gather(t) for t in ts]
        system = [a + jnp.where(eye, 127.0, 0.0) for a, _ in both]
        cross = [c[:1] for _, c in both]
        inv = [
            lax.rsqrt(jnp.sum(jnp.sum(a * a, axis=0, keepdims=True), axis=1, keepdims=True))
            for a in system
        ]
        w = each(lambda a, i: a * i, system, inv)
        root = None
        for step in range(3):
            ws = each(split, w)
            w2 = each(mul, ws, ws)
            w2s = each(split, w2)
            tail = each(lambda a, c: split(-0.5625 * a + 0.0625 * c), w, w2)
            high = each(mul, w2s, tail)
            q = each(
                lambda a, c, h: jnp.where(eye, 2.25, 0.0) - 2.4375 * a + 1.6875 * c + h, w, w2, high
            )
            qs = each(split, q)
            root = q if root is None else each(lambda a, r: mul(a, split(r)), qs, root)
            if step < 2:
                half = each(mul, ws, qs)
                w = each(lambda a, c: mul(split(a), c), half, qs)
        for u, t in enumerate(ts):
            r = root[u]
            col = jnp.sum(r * cross[u], axis=1, keepdims=True)
            row = jnp.sum(r * col, axis=0, keepdims=True) * inv[u]
            out[t] = (r * jnp.sqrt(127.0 * inv[u]) + row).astype(BF16)
        return carry

    lax.fori_loop(0, out.shape[0] // UNROLL, tiles, 0)


def update_kernel(info, tr, *refs):
    parts, outs = refs[:8], refs[8:]
    k = info[1]

    def tile(t, carry):
        b = 32 * k + t
        x = jnp.concatenate([r[b] for r in parts], axis=0).astype(F32)
        mean = jnp.sum(x, axis=0, keepdims=True) * (1.0 / 128.0)
        anomaly = (x - mean).astype(BF16)
        new = jnp.dot(tr[t], anomaly, preferred_element_type=F32) + mean
        new = new.astype(BF16)
        for i, o in enumerate(outs):
            o[t] = new[16 * i : 16 * i + 16]
        return carry

    lax.fori_loop(0, tr.shape[0], tile, 0, unroll=4)


def place_kernel(info, *refs):
    pieces, out, buf = refs[:8], refs[8], refs[9]
    z, k = info[0], info[1]
    for i, piece in enumerate(pieces):
        d, o = i % 4, i // 4
        zz = (z + d) % 4
        kk = k if o == 0 else 1 - k
        at = pl.multiple_of(64 * zz + 32 * kk, 32)
        for t in range(32):
            buf[i % 2, pl.ds(t, 16, stride=33), :] = piece[t].astype(F32)
        for m in range(16):
            out[m, pl.ds(at, 32), :] = buf[i % 2, 33 * m : 33 * m + 32, :].astype(BF16)


def vmem():
    return pl.BlockSpec(memory_space=pltpu.VMEM)


def smem():
    return pl.BlockSpec(memory_space=pltpu.SMEM)


def call(kernel, n_smem, args, outs, scratch=()):
    return pl.pallas_call(
        kernel,
        in_specs=[smem()] * n_smem + [vmem()] * (len(args) - n_smem),
        out_specs=jax.tree.map(lambda _: vmem(), outs),
        out_shape=outs,
        scratch_shapes=list(scratch),
        compiler_params=pltpu.CompilerParams(vmem_limit_bytes=48 * 1024 * 1024),
    )(*args)


def to_z(x, by):
    return lax.ppermute(x, "z", [(i, (i + by) % 4) for i in range(4)])


def to_core(x):
    return lax.ppermute(x, "k", [(0, 1), (1, 0)])


def to_side(x, d):
    n = lax.axis_size("cells")
    pairs = []
    for c in range(n):
        for z in range(4):
            zz = (z + d) % 4
            cc = (c + 1) % n if zz < 2 else (c - 1) % n
            pairs += [(8 * c + 2 * z + k, 8 * cc + 2 * zz + k) for k in range(2)]
    return lax.ppermute(x, ("cells", "z", "k"), pairs)


def home(x, d, o):
    pairs = [(2 * z + k, 2 * ((z - d) % 4) + (k ^ o)) for z in range(4) for k in range(2)]
    return lax.ppermute(x, MEM, pairs)


def per_device(bg, figures, spread, pixel, active, nbr):
    members, tiles, width = bg.shape
    groups = tiles // PACK
    z, k = lax.axis_index("z"), lax.axis_index("k")
    first = lax.axis_index("cells") * tiles + 64 * z + 32 * k
    info = jnp.stack([z, k, first, tiles * lax.axis_size("cells")]).astype(jnp.int32)
    half = groups // 2
    shape = lambda n: jax.ShapeDtypeStruct((n, members, width), BF16)
    sg, *rest = call(
        sense_kernel,
        1,
        (info, bg),
        (shape(groups),) + (shape(half),) * 4 + (shape(tiles // 4),) * 4,
        [pltpu.VMEM((members * (tiles + 1) + 7, width), F32)],
    )
    ends = [to_side(rest[d], d) for d in range(4)]
    own = [sg] + [to_z(sg, d) for d in (1, 2, 3)]
    state = [rest[4]] + [to_z(rest[4 + d], d) for d in (1, 2, 3)]
    live = jnp.arange(128, dtype=jnp.int32)[None, :] < active[:, None]
    w2 = jnp.where(live, 1.0 / spread, 0.0)
    de, near = call(
        cell_kernel,
        1,
        (info, pixel, w2, figures),
        (jax.ShapeDtypeStruct((2, groups, 128), F32), jax.ShapeDtypeStruct((2, half, 128), F32)),
    )
    dn = to_side(near, 0)
    own += [to_core(r) for r in own]
    ends += [to_core(r) for r in ends]
    state += [to_core(r) for r in state]
    own_nbr = lax.dynamic_slice_in_dim(nbr, 64 * z + 32 * k, 32, 0)
    transform = call(
        solve_kernel,
        2,
        (info, own_nbr, *own, *ends, de, dn),
        jax.ShapeDtypeStruct((32, 128, 128), BF16),
        [
            pltpu.VMEM((72, 128, 128), BF16),
            pltpu.VMEM((72, 128, 128), BF16),
            pltpu.VMEM((72, 128, 8), BF16),
        ],
    )
    outs = call(update_kernel, 1, (info, transform, *state), (shape(32),) * 8)
    back = [
        outs[i] if i == 0 else home(outs[i], i % 4, i // 4) for i in range(8)
    ]
    return call(
        place_kernel,
        1,
        (info, *back),
        jax.ShapeDtypeStruct((members, tiles, width), BF16),
        [pltpu.VMEM((2, 16 * 33, 128), F32)],
    )


def solution(mesh):
    finer = Mesh(mesh.devices.reshape(mesh.shape["cells"], 4, 2), ("cells", "z", "k"))
    placed = (
        P(MEM, "cells", None),
        P("cells", None),
        P("cells", None),
        P("cells", None),
        P("cells"),
        P("cells", None),
    )
    return jax.shard_map(
        per_device, mesh=finer, in_specs=placed, out_specs=P(MEM, "cells", None), check_vma=False
    )
```

```python
import jax
import jax.numpy as jnp
from jax import lax
from jax.experimental import pallas as pl
from jax.experimental.pallas import tpu as pltpu
from jax.sharding import Mesh
from jax.sharding import PartitionSpec as P

F32 = jnp.float32
BF16 = jnp.bfloat16
MEM = ("z", "k")
PACK = 4
UNROLL = 16


def lane_id(rows):
    return lax.broadcasted_iota(jnp.int32, (rows, 128), 1)


def sense_kernel(info, bg, sg, *refs):
    states, buf = refs[:8], refs[8]
    members, tiles, _ = bg.shape
    z, k = info[0], info[1]
    pitch = tiles + 1
    for m in range(members):
        buf[pl.ds(m * pitch, tiles), :] = bg[m].astype(F32)
    quarter = lane_id(members) >> 5
    chunk = tiles // 8
    for n, xd in enumerate(states):
        zone = 2 * ((z + n) % 4) + (k if n < 4 else 1 - k)

        def group(i, carry, xd=xd, zone=zone):
            row = None
            for q in range(PACK):
                x = buf[pl.ds(chunk * zone + PACK * i + q, members, stride=pitch), :]
                xd[PACK * i + q] = x.astype(BF16)
                s = x + 0.5 * pltpu.roll(x, 96, 1)
                s = s if q == 0 else pltpu.roll(s, 32 * q, 1)
                row = s if q == 0 else jnp.where(quarter == q, s, row)
            sg[(chunk // PACK) * zone + i] = row.astype(BF16)
            return carry

        lax.fori_loop(0, chunk // PACK, group, 0, unroll=4)


def window_kernel(info, sg, left, right, *outs):
    half = left.shape[0]
    z = info[0]
    for d, w in enumerate(outs):
        zz = (z + d) % 4

        @pl.when(zz < 2)
        def _():
            for i in range(16):
                w[i] = left[16 * zz + i]
            for j in range(4):
                src = 16 * zz + 16 * (j + 1) - half

                @pl.when(src < 0)
                def _():
                    for i in range(16):
                        w[16 * (j + 1) + i] = left[src + half + i]

                @pl.when(src >= 0)
                def _():
                    for i in range(16):
                        w[16 * (j + 1) + i] = sg[src + i]

        @pl.when(zz >= 2)
        def _():
            for j in range(5):
                src = 16 * zz + 16 * j - half

                @pl.when(src < 2 * half)
                def _():
                    for i in range(16):
                        w[16 * j + i] = sg[src + i]

                @pl.when(src >= 2 * half)
                def _():
                    for i in range(16):
                        w[16 * j + i] = right[src - 2 * half + i]


def cell_kernel(info, pix, w2, y, nbr, out, near, own_nbr):
    groups = pix.shape[0] // PACK

    def packed(ref, p):
        parts = [ref[pl.ds(2 * p + h, groups, stride=PACK), :] for h in range(2)]
        return jnp.concatenate(parts, axis=0).astype(F32).T

    cols = [[], []]
    for p in range(2):
        pt = packed(pix, p)
        wt = packed(w2, p)
        yt = packed(y, p) * wt
        d, e = [], []
        for c in range(32):
            hit = pt == float(c)
            d.append(jnp.sum(jnp.where(hit, wt, 0.0), axis=0, keepdims=True))
            e.append(jnp.sum(jnp.where(hit, yt, 0.0), axis=0, keepdims=True))
        for i, rows in enumerate((d, e)):
            block = jnp.concatenate(rows, axis=0)
            cols[i] += [block, pltpu.roll(block, 64, 1)]
    own_nbr[...] = nbr[pl.ds(pl.multiple_of(64 * info[0] + 32 * info[1], 32), 32), :]
    at = pl.multiple_of(jnp.where(info[0] < 2, 32, 0), 32)
    for i in range(2):
        out[i] = jnp.concatenate(cols[i], axis=0).T[:groups]
        near[i] = out[i, pl.ds(at, 32), :]


def pair_dot(left, right):
    zero = jnp.zeros((128, 128), BF16)
    top = jnp.concatenate([right[:, :128], zero], axis=1)
    low = jnp.concatenate([zero, right[:, 128:]], axis=1)
    both = jnp.concatenate([top, low], axis=0)
    return jnp.dot(left, both, preferred_element_type=F32)


def each(f, *lists):
    return [f(*a) for a in zip(*lists)]


def narrow(a):
    return a.astype(BF16)


def solve_kernel(info, nbr, *refs):
    parts, (de, dn, out, gt, lt, ks) = refs[:8], refs[8:]
    z, k, first, total = info[0], info[1], info[2], info[3]
    reach = 128
    start = 16 * z - 32 + 8 * k
    low = z < 2
    n_end = jnp.where(low, -start, start + 8)
    end_at = jnp.where(low, 32 + start, 0)
    end_to = jnp.where(low, 0, 64 - start)
    own_at = jnp.where(low, 0, start)
    own_to = jnp.where(low, -start, 0)
    mine = lax.broadcasted_iota(jnp.int32, (8, 128), 0) == (lane_id(8) >> 5)

    def center(table, b, g):
        x = jnp.concatenate([r[8 * k + g] for r in parts], axis=0).astype(F32)
        mean = jnp.sum(x, axis=0, keepdims=True) * (1.0 / 128.0)
        d = table[0, pl.ds(b, 1), :]
        e = table[1, pl.ds(b, 1), :] - d * mean
        a = x - mean
        turned = a.astype(BF16).T
        gt[g] = turned
        lt[g] = (a * d).astype(BF16).T
        ks[pl.ds(8 * g, 8), :] = jnp.dot(
            jnp.where(mine, e, 0.0).astype(BF16), turned, preferred_element_type=F32
        )

    def own_eight(j, carry):
        for i in range(8):
            center(de, own_at + 8 * j + i, own_to + 8 * j + i)
        return carry

    def end_eight(j, carry):
        for i in range(8):
            center(dn, end_at + 8 * j + i, end_to + 8 * j + i)
        return carry

    lax.fori_loop(0, (gt.shape[0] - n_end) // 8, own_eight, 0)
    lax.fori_loop(0, n_end // 8, end_eight, 0)
    eye = lax.broadcasted_iota(jnp.int32, (128, 128), 0) == lane_id(128)

    def gather(t):
        lhs, rhs, cross = [], [], None
        for n in range(5):
            if n == 0:
                loc, tap = t + reach, None
            else:
                gap = nbr[t, n - 1] - (first + t)
                gap = jnp.where(gap < 0, gap + total, gap)
                gap = jnp.where(gap > total // 2, gap - total, gap)
                loc = t + reach + gap
                tap = 1.0 - jnp.abs(gap).astype(F32) * (1.0 / (reach + 1.0))
            g = loc // PACK
            at = pl.multiple_of(32 * (loc % PACK), 32)
            rhs.append(gt[g, pl.ds(at, 32), :])
            v = lt[g, pl.ds(at, 32), :]
            c = ks[pl.ds(8 * g + loc % PACK, 1), :]
            lhs.append(v if tap is None else (v.astype(F32) * tap).astype(BF16))
            cross = c if n == 0 else cross + tap * c
        cat = lambda v: jnp.concatenate(v, axis=0)
        dims = (((0,), (0,)), ((), ()))
        gram = lax.dot_general(cat(lhs), cat(rhs), dims, preferred_element_type=F32)
        return gram, cross

    def prepare(t):
        gram, cross = gather(t)
        total_sq = lambda a: jnp.sum(jnp.sum(a, axis=0, keepdims=True), axis=1, keepdims=True)
        diag = jnp.where(eye, gram, 0.0)
        system = gram + jnp.where(eye, 127.0, 0.0)
        inv = lax.rsqrt(total_sq(system * system))
        mid = 127.0 + total_sq(diag) * (1.0 / 128.0)
        rest = (system - jnp.where(eye, mid, 0.0)) * inv
        wide = lambda v: jnp.broadcast_to(v, (1, 128))
        return rest, wide(mid * inv), wide(inv), cross

    unit = jnp.where(eye, 1.0, 0.0)
    unit = narrow(jnp.concatenate([unit, unit], axis=1))

    def tiles(b, carry):
        ts = [b * UNROLL + u for u in range(UNROLL)]
        ready = [prepare(t) for t in ts]
        pairs = range(UNROLL // 2)
        wide = lambda j: [
            jnp.concatenate([ready[2 * p][j], ready[2 * p + 1][j]], axis=1) for p in pairs
        ]
        v, al = wide(0), wide(1)
        root = rho = None
        for step in range(3):
            vs = each(narrow, v)
            sq = each(pair_dot, vs, vs)
            be = each(lambda a: a * (0.0625 * a - 0.5625), al)
            cx = each(lambda a, c: 1.6875 + c + 0.0625 * a * a, al, be)
            c1 = each(lambda a, c: 2.0 * a * c - 2.4375 - 0.5625 * a * a, al, cx)
            ga = each(lambda a, c: 2.25 + a * (1.6875 * a - 2.4375) + a * a * c, al, be)
            xs, ys, lin = [], [], []
            for m, p, a, i, j in zip(v, sq, al, c1, cx):
                n = narrow(m)
                x = narrow(2.0 * a) * n + narrow(p)
                xs.append(x)
                ys.append(0.0625 * x - 0.5625 * n)
                lin.append(i * m + j * p)
            high = each(pair_dot, xs, ys)
            q = each(lambda m, h: m + h, lin, high)
            qs = each(narrow, q)

            def times(m, a):
                prod = each(lambda i, c, r: pair_dot(narrow(i) + unit * narrow(c), r), m, a, qs)
                rest = each(lambda g, j, d: g * j + d, ga, m, prod)
                return rest, each(lambda i, g: i * g, a, ga)

            root, rho = (q, ga) if root is None else times(root, rho)
            if step < 2:
                v, al = times(*times(v, al))
        for u, t in enumerate(ts):
            _, _, inv, cross = ready[u]
            at = 128 * (u % 2)
            r = root[u // 2][:, at : at + 128]
            r = r + jnp.where(eye, rho[u // 2][:, at : at + 128], 0.0)
            col = jnp.sum(r * cross, axis=1, keepdims=True)
            row = jnp.sum(r * col, axis=0, keepdims=True) * inv
            out[t] = (r * jnp.sqrt(127.0 * inv) + row).astype(BF16)
        return carry

    lax.fori_loop(0, out.shape[0] // UNROLL, tiles, 0)


def update_kernel(info, tr, *refs):
    parts, outs = refs[:8], refs[8:]

    def tile(t, carry):
        x = jnp.concatenate([r[t] for r in parts], axis=0).astype(F32)
        mean = jnp.sum(x, axis=0, keepdims=True) * (1.0 / 128.0)
        anomaly = (x - mean).astype(BF16)
        new = jnp.dot(tr[t], anomaly, preferred_element_type=F32) + mean
        new = new.astype(BF16)
        for i, o in enumerate(outs):
            o[t] = new[16 * i : 16 * i + 16]
        return carry

    lax.fori_loop(0, tr.shape[0], tile, 0, unroll=8)


def place_kernel(info, *refs):
    pieces, out, buf = refs[:8], refs[8], refs[9]
    z, k = info[0], info[1]
    for i, piece in enumerate(pieces):
        d, o = i % 4, i // 4
        zz = (z + d) % 4
        kk = k if o == 0 else 1 - k
        at = pl.multiple_of(64 * zz + 32 * kk, 32)
        for t in range(32):
            buf[i % 2, pl.ds(t, 16, stride=33), :] = piece[t].astype(F32)
        for m in range(16):
            out[m, pl.ds(at, 32), :] = buf[i % 2, 33 * m : 33 * m + 32, :].astype(BF16)


def vmem():
    return pl.BlockSpec(memory_space=pltpu.VMEM)


def smem():
    return pl.BlockSpec(memory_space=pltpu.SMEM)


def call(kernel, n_smem, args, outs, scratch=(), mib=12):
    return pl.pallas_call(
        kernel,
        in_specs=[smem()] * n_smem + [vmem()] * (len(args) - n_smem),
        out_specs=jax.tree.map(lambda _: vmem(), outs),
        out_shape=outs,
        scratch_shapes=list(scratch),
        compiler_params=pltpu.CompilerParams(vmem_limit_bytes=mib * 1024 * 1024),
    )(*args)


def to_z(x, by):
    return lax.ppermute(x, "z", [(i, (i + by) % 4) for i in range(4)])


def to_core(x):
    return lax.ppermute(x, "k", [(0, 1), (1, 0)])


def to_cells(x, by):
    n = lax.axis_size("cells")
    return lax.ppermute(x, "cells", [(i, (i + by) % n) for i in range(n)])


def to_side(x, d):
    n = lax.axis_size("cells")
    pairs = []
    for c in range(n):
        for z in range(4):
            zz = (z + d) % 4
            cc = (c + 1) % n if zz < 2 else (c - 1) % n
            pairs += [(8 * c + 2 * z + k, 8 * cc + 2 * zz + k) for k in range(2)]
    return lax.ppermute(x, ("cells", "z", "k"), pairs)


def away(x, d, o):
    pairs = [(2 * z + k, 2 * ((z + d) % 4) + (k ^ o)) for z in range(4) for k in range(2)]
    return lax.ppermute(x, MEM, pairs)


def home(x, d, o):
    pairs = [(2 * z + k, 2 * ((z - d) % 4) + (k ^ o)) for z in range(4) for k in range(2)]
    return lax.ppermute(x, MEM, pairs)


def analysis(bg, figures, spread, pixel, active, nbr):
    members, tiles, width = bg.shape
    groups = tiles // PACK
    z, k = lax.axis_index("z"), lax.axis_index("k")
    first = lax.axis_index("cells") * tiles + 64 * z + 32 * k
    info = jnp.stack([z, k, first, tiles * lax.axis_size("cells")]).astype(jnp.int32)
    half = groups // 2
    shape = lambda n: jax.ShapeDtypeStruct((n, members, width), BF16)
    sg, *rest = call(
        sense_kernel,
        1,
        (info, bg),
        (shape(groups),) + (shape(tiles // 8),) * 8,
        [pltpu.VMEM((members * (tiles + 1) + 7, width), F32)],
    )
    left = to_cells(sg[half:], 1)
    right = to_cells(sg[:half], -1)
    windows = call(window_kernel, 1, (info, sg, left, right), (shape(80),) * 4)
    own = [windows[0]] + [to_z(windows[d], d) for d in (1, 2, 3)]
    state = [rest[i] if i == 0 else away(rest[i], i % 4, i // 4) for i in range(8)]
    live = jnp.arange(128, dtype=jnp.int32)[None, :] < active[:, None]
    w2 = jnp.where(live, 1.0 / spread, 0.0)
    de, near, own_nbr = call(
        cell_kernel,
        1,
        (info, pixel, w2, figures, nbr),
        (
            jax.ShapeDtypeStruct((2, groups, 128), F32),
            jax.ShapeDtypeStruct((2, half, 128), F32),
            jax.ShapeDtypeStruct((32, 4), jnp.int32),
        ),
    )
    dn = to_side(near, 0)
    own += [to_core(r) for r in own]
    transform = call(
        solve_kernel,
        2,
        (info, own_nbr, *own, de, dn),
        jax.ShapeDtypeStruct((32, 128, 128), BF16),
        [
            pltpu.VMEM((72, 128, 128), BF16),
            pltpu.VMEM((72, 128, 128), BF16),
            pltpu.VMEM((8 * 72, 128), F32),
        ],
        40,
    )
    outs = call(update_kernel, 1, (info, transform, *state), (shape(32),) * 8)
    back = [
        outs[i] if i == 0 else home(outs[i], i % 4, i // 4) for i in range(8)
    ]
    return call(
        place_kernel,
        1,
        (info, *back),
        jax.ShapeDtypeStruct((members, tiles, width), BF16),
        [pltpu.VMEM((2, 16 * 33, 128), F32)],
    )


def solution(mesh):
    finer = Mesh(mesh.devices.reshape(mesh.shape["cells"], 4, 2), ("cells", "z", "k"))
    placed = (
        P(MEM, "cells", None),
        P("cells", None),
        P("cells", None),
        P("cells", None),
        P("cells"),
        P("cells", None),
    )
    return jax.shard_map(
        analysis, mesh=finer, in_specs=placed, out_specs=P(MEM, "cells", None), check_vma=False
    )
```

```python
import jax
import jax.numpy as jnp
from jax import lax
from jax.experimental import pallas as pl
from jax.experimental.pallas import tpu as pltpu
from jax.sharding import Mesh
from jax.sharding import PartitionSpec as P

F32 = jnp.float32
BF16 = jnp.bfloat16
MEM = ("z", "k")
PACK = 4
UNROLL = 16


def lane_id(rows):
    return lax.broadcasted_iota(jnp.int32, (rows, 128), 1)


def sense_kernel(info, bg, sg, *refs):
    keeps, (give, buf) = refs[:4], refs[4:]
    members, tiles, _ = bg.shape
    z, k = info[0], info[1]
    pitch = tiles + 1
    row = lax.broadcasted_iota(jnp.int32, (128 * PACK, 128), 0)
    lane, q = row & 127, row >> 7
    goal = lane_id(128 * PACK) - 32 * q
    pick = jnp.where((lane == goal) & (lane < 32), 1.0, 0.0)
    pick = pick + jnp.where((lane - 32 == goal) & (lane >= 32) & (lane < 64), 0.5, 0.0)
    pick = pick.astype(BF16)
    for m in range(members):
        buf[pl.ds(m * pitch, tiles), :] = bg[m].astype(F32)
    chunk = tiles // 8
    for n in range(8):
        zone = 2 * ((z + n) % 4) + (k if n < 4 else 1 - k)
        xd, skip = (keeps[n], 0) if n < 4 else (give, chunk * (n - 4))
        rows = []
        for i in range(chunk // PACK):
            group = []
            for q in range(PACK):
                at = chunk * zone + PACK * i + q
                x = buf[pl.ds(at, members, stride=pitch), :].astype(BF16)
                xd[skip + PACK * i + q] = x
                group.append(x)
            rows.append(jnp.concatenate(group, axis=1))
        sensed = jnp.dot(jnp.concatenate(rows, axis=0), pick, preferred_element_type=F32)
        sensed = sensed.astype(BF16)
        for i in range(chunk // PACK):
            sg[(chunk // PACK) * zone + i] = sensed[members * i : members * (i + 1)]


def both_kernel(k1, k2, k3, given, *outs):
    for d, (keep, both) in enumerate(zip((k1, k2, k3), outs), 1):
        n = keep.shape[0]
        for i in range(n):
            both[i] = keep[i]
            both[n + i] = given[n * d + i]


def window_kernel(info, sg, left, right, *outs):
    half = left.shape[0]
    z = info[0]
    for d, w in enumerate(outs):
        zz = (z + d) % 4

        @pl.when(zz < 2)
        def _():
            for i in range(16):
                w[i] = left[16 * zz + i]
            for j in range(4):
                src = 16 * zz + 16 * (j + 1) - half

                @pl.when(src < 0)
                def _():
                    for i in range(16):
                        w[16 * (j + 1) + i] = left[src + half + i]

                @pl.when(src >= 0)
                def _():
                    for i in range(16):
                        w[16 * (j + 1) + i] = sg[src + i]

        @pl.when(zz >= 2)
        def _():
            for j in range(5):
                src = 16 * zz + 16 * j - half

                @pl.when(src < 2 * half)
                def _():
                    for i in range(16):
                        w[16 * j + i] = sg[src + i]

                @pl.when(src >= 2 * half)
                def _():
                    for i in range(16):
                        w[16 * j + i] = right[src - 2 * half + i]


def obs_kernel(info, pix, spread, y, active, w2, side):
    half = pix.shape[0] // 2
    counts = jnp.concatenate([active[...]] * 4, axis=0).astype(F32).T
    slot = lane_id(half).astype(F32)
    for h in range(2):
        rows = pl.ds(half * h, half)
        w2[rows, :] = jnp.where(slot < counts[:, h : h + 1], 1.0 / spread[rows, :], 0.0)
    rows = pl.ds(pl.multiple_of(jnp.where(info[0] < 2, half, 0), half), half)
    side[0] = pix[rows, :].astype(F32)
    side[1] = w2[rows, :]
    side[2] = y[rows, :]


def cell_kernel(info, pix, w2, y, side, nbr, out, near, own_nbr):
    groups = pix.shape[0] // PACK

    def sums(pt, wt, yt):
        yt = yt * wt
        d, e = [], []
        for c in range(32):
            hit = pt == float(c)
            d.append(jnp.sum(jnp.where(hit, wt, 0.0), axis=0, keepdims=True))
            e.append(jnp.sum(jnp.where(hit, yt, 0.0), axis=0, keepdims=True))
        return jnp.concatenate(d, axis=0), jnp.concatenate(e, axis=0)

    def packed(ref, n, qs):
        parts = [ref[pl.ds(q, n, stride=PACK), :] for q in qs]
        return jnp.concatenate(parts, axis=0).astype(F32).T

    cols = [[], []]
    for p in range(2):
        qs = (2 * p, 2 * p + 1)
        for i, block in enumerate(sums(*[packed(r, groups, qs) for r in (pix, w2, y)])):
            cols[i] += [block, pltpu.roll(block, 64, 1)]
    for i in range(2):
        out[i] = jnp.concatenate(cols[i], axis=0).T[:groups]
    some = sums(*[packed(side.at[i], groups // 2, range(PACK)) for i in range(3)])
    for i, block in enumerate(some):
        turned = [block] + [pltpu.roll(block, 128 - 32 * q, 1) for q in range(1, PACK)]
        near[i] = jnp.concatenate(turned, axis=0).T[: groups // 2]
    own_nbr[...] = nbr[pl.ds(pl.multiple_of(64 * info[0] + 32 * info[1], 32), 32), :]


def pair_dot(left, right):
    zero = jnp.zeros((128, 128), BF16)
    top = jnp.concatenate([right[:, :128], zero], axis=1)
    low = jnp.concatenate([zero, right[:, 128:]], axis=1)
    both = jnp.concatenate([top, low], axis=0)
    return jnp.dot(left, both, preferred_element_type=F32)


def each(f, *lists):
    return [f(*a) for a in zip(*lists)]


def narrow(a):
    return a.astype(BF16)


def solve_kernel(info, nbr, *refs):
    parts, (de, dn, out, gt, lt, ks) = refs[:8], refs[8:]
    z, k, first, total = info[0], info[1], info[2], info[3]
    reach = 128
    start = 16 * z - 32 + 8 * k
    low = z < 2
    n_end = jnp.where(low, -start, start + 8)
    end_at = jnp.where(low, 32 + start, 0)
    end_to = jnp.where(low, 0, 64 - start)
    own_at = jnp.where(low, 0, start)
    own_to = jnp.where(low, -start, 0)
    mine = lax.broadcasted_iota(jnp.int32, (8, 128), 0) == (lane_id(8) >> 5)

    def center(table, b, g):
        x = jnp.concatenate([r[8 * k + g] for r in parts], axis=0).astype(F32)
        mean = jnp.sum(x, axis=0, keepdims=True) * (1.0 / 128.0)
        d = table[0, pl.ds(b, 1), :]
        e = table[1, pl.ds(b, 1), :] - d * mean
        a = x - mean
        turned = a.astype(BF16).T
        gt[g] = turned
        lt[g] = (a * d).astype(BF16).T
        ks[pl.ds(8 * g, 8), :] = jnp.dot(
            jnp.where(mine, e, 0.0).astype(BF16), turned, preferred_element_type=F32
        )

    def own_eight(j, carry):
        for i in range(8):
            center(de, own_at + 8 * j + i, own_to + 8 * j + i)
        return carry

    def end_eight(j, carry):
        for i in range(8):
            center(dn, end_at + 8 * j + i, end_to + 8 * j + i)
        return carry

    lax.fori_loop(0, (gt.shape[0] - n_end) // 8, own_eight, 0)
    lax.fori_loop(0, n_end // 8, end_eight, 0)
    eye = lax.broadcasted_iota(jnp.int32, (128, 128), 0) == lane_id(128)

    def gather(t):
        lhs, rhs, cross = [], [], None
        for n in range(5):
            if n == 0:
                loc, tap = t + reach, None
            else:
                gap = nbr[t, n - 1] - (first + t)
                gap = jnp.where(gap < 0, gap + total, gap)
                gap = jnp.where(gap > total // 2, gap - total, gap)
                loc = t + reach + gap
                tap = 1.0 - jnp.abs(gap).astype(F32) * (1.0 / (reach + 1.0))
            g = loc // PACK
            at = pl.multiple_of(32 * (loc % PACK), 32)
            rhs.append(gt[g, pl.ds(at, 32), :])
            v = lt[g, pl.ds(at, 32), :]
            c = ks[pl.ds(8 * g + loc % PACK, 1), :]
            lhs.append(v if tap is None else (v.astype(F32) * tap).astype(BF16))
            cross = c if n == 0 else cross + tap * c
        cat = lambda v: jnp.concatenate(v, axis=0)
        dims = (((0,), (0,)), ((), ()))
        gram = lax.dot_general(cat(lhs), cat(rhs), dims, preferred_element_type=F32)
        return gram, cross

    def prepare(t):
        gram, cross = gather(t)
        total_sq = lambda a: jnp.sum(jnp.sum(a, axis=0, keepdims=True), axis=1, keepdims=True)
        diag = jnp.where(eye, gram, 0.0)
        system = gram + jnp.where(eye, 127.0, 0.0)
        inv = lax.rsqrt(total_sq(system * system))
        mid = 127.0 + total_sq(diag) * (1.0 / 128.0)
        rest = (system - jnp.where(eye, mid, 0.0)) * inv
        wide = lambda v: jnp.broadcast_to(v, (1, 128))
        return rest, wide(mid * inv), wide(inv), cross

    unit = jnp.where(eye, 1.0, 0.0)
    unit = narrow(jnp.concatenate([unit, unit], axis=1))

    def tiles(b, carry):
        ts = [b * UNROLL + u for u in range(UNROLL)]
        ready = [prepare(t) for t in ts]
        pairs = range(UNROLL // 2)
        wide = lambda j: [
            jnp.concatenate([ready[2 * p][j], ready[2 * p + 1][j]], axis=1) for p in pairs
        ]
        v, al = wide(0), wide(1)
        root = rho = None
        for step in range(3):
            vs = each(narrow, v)
            sq = each(pair_dot, vs, vs)
            be = each(lambda a: a * (0.0625 * a - 0.5625), al)
            cx = each(lambda a, c: 1.6875 + c + 0.0625 * a * a, al, be)
            c1 = each(lambda a, c: 2.0 * a * c - 2.4375 - 0.5625 * a * a, al, cx)
            ga = each(lambda a, c: 2.25 + a * (1.6875 * a - 2.4375) + a * a * c, al, be)
            xs, ys, lin = [], [], []
            for m, p, a, i, j in zip(v, sq, al, c1, cx):
                n = narrow(m)
                x = narrow(2.0 * a) * n + narrow(p)
                xs.append(x)
                ys.append(0.0625 * x - 0.5625 * n)
                lin.append(i * m + j * p)
            high = each(pair_dot, xs, ys)
            q = each(lambda m, h: m + h, lin, high)
            qs = each(narrow, q)

            def times(m, a):
                prod = each(lambda i, c, r: pair_dot(narrow(i) + unit * narrow(c), r), m, a, qs)
                rest = each(lambda g, j, d: g * j + d, ga, m, prod)
                return rest, each(lambda i, g: i * g, a, ga)

            root, rho = (q, ga) if root is None else times(root, rho)
            if step < 2:
                v, al = times(*times(v, al))
        for u, t in enumerate(ts):
            _, _, inv, cross = ready[u]
            at = 128 * (u % 2)
            r = root[u // 2][:, at : at + 128]
            r = r + jnp.where(eye, rho[u // 2][:, at : at + 128], 0.0)
            col = jnp.sum(r * cross, axis=1, keepdims=True)
            row = jnp.sum(r * col, axis=0, keepdims=True) * inv
            out[t] = (r * jnp.sqrt(127.0 * inv) + row).astype(BF16)
        return carry

    lax.fori_loop(0, out.shape[0] // UNROLL, tiles, 0)


def update_kernel(info, tr, keep, given, s1, s2, s3, *outs):
    n = tr.shape[0]

    def tile(t, carry):
        parts = [keep[t], s1[t], s2[t], s3[t], given[t], s1[n + t], s2[n + t], s3[n + t]]
        x = jnp.concatenate(parts, axis=0).astype(F32)
        mean = jnp.sum(x, axis=0, keepdims=True) * (1.0 / 128.0)
        anomaly = (x - mean).astype(BF16)
        new = jnp.dot(tr[t], anomaly, preferred_element_type=F32) + mean
        new = new.astype(BF16)
        for i, o in enumerate(outs):
            o[t] = new[16 * i : 16 * i + 16]
        return carry

    lax.fori_loop(0, n, tile, 0, unroll=8)


def place_kernel(info, *refs):
    pieces, out, buf = refs[:8], refs[8], refs[9]
    z, k = info[0], info[1]
    for i, piece in enumerate(pieces):
        d, o = i % 4, i // 4
        zz = (z + d) % 4
        kk = k if o == 0 else 1 - k
        at = pl.multiple_of(64 * zz + 32 * kk, 32)
        for t in range(32):
            buf[i % 2, pl.ds(t, 16, stride=33), :] = piece[t].astype(F32)
        for m in range(16):
            out[m, pl.ds(at, 32), :] = buf[i % 2, 33 * m : 33 * m + 32, :].astype(BF16)


def vmem():
    return pl.BlockSpec(memory_space=pltpu.VMEM)


def smem():
    return pl.BlockSpec(memory_space=pltpu.SMEM)


def call(kernel, n_smem, args, outs, scratch=(), mib=12, specs=None):
    return pl.pallas_call(
        kernel,
        in_specs=[smem()] * n_smem + list(specs or [vmem()] * (len(args) - n_smem)),
        out_specs=jax.tree.map(lambda _: vmem(), outs),
        out_shape=outs,
        scratch_shapes=list(scratch),
        compiler_params=pltpu.CompilerParams(vmem_limit_bytes=mib * 1024 * 1024),
    )(*args)


def to_z(x, by):
    return lax.ppermute(x, "z", [(i, (i + by) % 4) for i in range(4)])


def to_core(x):
    return lax.ppermute(x, "k", [(0, 1), (1, 0)])


def to_cells(x, by):
    n = lax.axis_size("cells")
    return lax.ppermute(x, "cells", [(i, (i + by) % n) for i in range(n)])


def to_side(x, d):
    n = lax.axis_size("cells")
    pairs = []
    for c in range(n):
        for z in range(4):
            zz = (z + d) % 4
            cc = (c + 1) % n if zz < 2 else (c - 1) % n
            pairs += [(8 * c + 2 * z + k, 8 * cc + 2 * zz + k) for k in range(2)]
    return lax.ppermute(x, ("cells", "z", "k"), pairs)


def home(x, d, o):
    pairs = [(2 * z + k, 2 * ((z - d) % 4) + (k ^ o)) for z in range(4) for k in range(2)]
    return lax.ppermute(x, MEM, pairs)


def analysis(bg, figures, spread, pixel, active, nbr):
    members, tiles, width = bg.shape
    groups = tiles // PACK
    z, k = lax.axis_index("z"), lax.axis_index("k")
    first = lax.axis_index("cells") * tiles + 64 * z + 32 * k
    info = jnp.stack([z, k, first, tiles * lax.axis_size("cells")]).astype(jnp.int32)
    half = groups // 2
    shape = lambda n: jax.ShapeDtypeStruct((n, members, width), BF16)
    sg, *rest = call(
        sense_kernel,
        1,
        (info, bg),
        (shape(groups),) + (shape(tiles // 8),) * 4 + (shape(tiles // 2),),
        [pltpu.VMEM((members * (tiles + 1) + 7, width), F32)],
    )
    left = to_cells(sg[half:], 1)
    right = to_cells(sg[:half], -1)
    keep, give = rest[:4], rest[4]
    given = to_core(give)
    windows = call(
        window_kernel,
        1,
        (info, sg, left, right),
        (shape(80),) * 4,
    )
    own = [windows[0]] + [to_z(windows[d], d) for d in (1, 2, 3)]
    both = call(both_kernel, 0, (*keep[1:], given), (shape(tiles // 4),) * 3)
    state = [to_z(both[d - 1], d) for d in (1, 2, 3)]
    w2, side = call(
        obs_kernel,
        1,
        (info, pixel, spread, figures, active.reshape(2, tiles // 2)),
        (jax.ShapeDtypeStruct((tiles, 128), F32), jax.ShapeDtypeStruct((3, tiles // 2, 128), F32)),
    )
    side = to_side(side, 0)
    de, near, own_nbr = call(
        cell_kernel,
        1,
        (info, pixel, w2, figures, side, nbr),
        (
            jax.ShapeDtypeStruct((2, groups, 128), F32),
            jax.ShapeDtypeStruct((2, half, 128), F32),
            jax.ShapeDtypeStruct((32, 4), jnp.int32),
        ),
    )
    own += [to_core(r) for r in own]
    transform = call(
        solve_kernel,
        2,
        (info, own_nbr, *own, de, near),
        jax.ShapeDtypeStruct((32, 128, 128), BF16),
        [
            pltpu.VMEM((72, 128, 128), BF16),
            pltpu.VMEM((72, 128, 128), BF16),
            pltpu.VMEM((8 * 72, 128), F32),
        ],
        40,
    )
    outs = call(update_kernel, 1, (info, transform, keep[0], given, *state), (shape(32),) * 8)
    back = [
        outs[i] if i == 0 else home(outs[i], i % 4, i // 4) for i in range(8)
    ]
    return call(
        place_kernel,
        1,
        (info, *back),
        jax.ShapeDtypeStruct((members, tiles, width), BF16),
        [pltpu.VMEM((2, 16 * 33, 128), F32)],
    )


def solution(mesh):
    finer = Mesh(mesh.devices.reshape(mesh.shape["cells"], 4, 2), ("cells", "z", "k"))
    placed = (
        P(MEM, "cells", None),
        P("cells", None),
        P("cells", None),
        P("cells", None),
        P("cells"),
        P("cells", None),
    )
    return jax.shard_map(
        analysis, mesh=finer, in_specs=placed, out_specs=P(MEM, "cells", None), check_vma=False
    )
```

```python
import jax
import jax.numpy as jnp
from jax import lax
from jax.experimental import pallas as pl
from jax.experimental.pallas import tpu as pltpu
from jax.sharding import Mesh
from jax.sharding import PartitionSpec as P

F32 = jnp.float32
BF16 = jnp.bfloat16
MEM = ("z", "k")
PACK = 4
UNROLL = 16


def lane_id(rows):
    return lax.broadcasted_iota(jnp.int32, (rows, 128), 1)


def sense_kernel(info, bg, sg, *refs):
    keeps, (give, buf) = refs[:4], refs[4:]
    members, tiles, _ = bg.shape
    z, k = info[0], info[1]
    pitch = tiles + 1
    row = lax.broadcasted_iota(jnp.int32, (128 * PACK, 128), 0)
    lane, q = row & 127, row >> 7
    goal = lane_id(128 * PACK) - 32 * q
    pick = jnp.where((lane == goal) & (lane < 32), 1.0, 0.0)
    pick = pick + jnp.where((lane - 32 == goal) & (lane >= 32) & (lane < 64), 0.5, 0.0)
    pick = pick.astype(BF16)
    for m in range(members):
        buf[pl.ds(m * pitch, tiles), :] = bg[m].astype(F32)
    chunk = tiles // 8
    for n in range(8):
        zone = 2 * ((z + n) % 4) + (k if n < 4 else 1 - k)
        xd, skip = (keeps[n], 0) if n < 4 else (give, chunk * (n - 4))
        rows = []
        for i in range(chunk // PACK):
            group = []
            for q in range(PACK):
                at = chunk * zone + PACK * i + q
                x = buf[pl.ds(at, members, stride=pitch), :].astype(BF16)
                xd[skip + PACK * i + q] = x
                group.append(x)
            rows.append(jnp.concatenate(group, axis=1))
        sensed = jnp.dot(jnp.concatenate(rows, axis=0), pick, preferred_element_type=F32)
        sensed = sensed.astype(BF16)
        for i in range(chunk // PACK):
            sg[(chunk // PACK) * zone + i] = sensed[members * i : members * (i + 1)]


def both_kernel(k1, k2, k3, given, *outs):
    for d, (keep, both) in enumerate(zip((k1, k2, k3), outs), 1):
        n = keep.shape[0]
        for i in range(n):
            both[i] = keep[i]
            both[n + i] = given[n * d + i]


def pick_kernel(info, left, right, *outs):
    for d, end in enumerate(outs):
        low = (info[0] + d) % 4 < 2

        @pl.when(low)
        def _():
            for i in range(left.shape[0]):
                end[i] = left[i]

        @pl.when(jnp.logical_not(low))
        def _():
            for i in range(left.shape[0]):
                end[i] = right[i]


def cell_kernel(info, pix, spread, y, active, nbr, out, near, own_nbr, w2):
    groups = pix.shape[0] // PACK
    half = pix.shape[0] // 2
    counts = jnp.concatenate([active[...]] * 4, axis=0).astype(F32).T
    slot = lane_id(half).astype(F32)
    for h in range(2):
        rows = pl.ds(half * h, half)
        w2[rows, :] = jnp.where(slot < counts[:, h : h + 1], 1.0 / spread[rows, :], 0.0)

    def packed(ref, p):
        parts = [ref[pl.ds(2 * p + h, groups, stride=PACK), :] for h in range(2)]
        return jnp.concatenate(parts, axis=0).astype(F32).T

    cols = [[], []]
    for p in range(2):
        pt = packed(pix, p)
        wt = packed(w2, p)
        yt = packed(y, p) * wt
        d, e = [], []
        for c in range(32):
            hit = pt == float(c)
            d.append(jnp.sum(jnp.where(hit, wt, 0.0), axis=0, keepdims=True))
            e.append(jnp.sum(jnp.where(hit, yt, 0.0), axis=0, keepdims=True))
        for i, rows in enumerate((d, e)):
            block = jnp.concatenate(rows, axis=0)
            cols[i] += [block, pltpu.roll(block, 64, 1)]
    at = pl.multiple_of(jnp.where(info[0] < 2, 32, 0), 32)
    for i in range(2):
        out[i] = jnp.concatenate(cols[i], axis=0).T[:groups]
        near[i] = out[i, pl.ds(at, 32), :]
    own_nbr[...] = nbr[pl.ds(pl.multiple_of(64 * info[0] + 32 * info[1], 32), 32), :]


def pair_dot(left, right):
    zero = jnp.zeros((128, 128), BF16)
    top = jnp.concatenate([right[:, :128], zero], axis=1)
    low = jnp.concatenate([zero, right[:, 128:]], axis=1)
    both = jnp.concatenate([top, low], axis=0)
    return jnp.dot(left, both, preferred_element_type=F32)


def each(f, *lists):
    return [f(*a) for a in zip(*lists)]


def narrow(a):
    return a.astype(BF16)


def solve_kernel(info, nbr, *refs):
    own, ends, (de, dn, out, gt, lt, ks) = refs[:8], refs[8:16], refs[16:]
    z, k, first, total = info[0], info[1], info[2], info[3]
    reach = 128
    start = 16 * z - 32 + 8 * k
    low = z < 2
    n_end = jnp.where(low, -start, start + 8)
    end_at = jnp.where(low, 32 + start, 0)
    end_to = jnp.where(low, 0, 64 - start)
    own_at = jnp.where(low, 0, start)
    own_to = jnp.where(low, -start, 0)
    mine = lax.broadcasted_iota(jnp.int32, (8, 128), 0) == (lane_id(8) >> 5)

    def center(src, table, b, g):
        x = jnp.concatenate([r[b] for r in src], axis=0).astype(F32)
        mean = jnp.sum(x, axis=0, keepdims=True) * (1.0 / 128.0)
        d = table[0, pl.ds(b, 1), :]
        e = table[1, pl.ds(b, 1), :] - d * mean
        a = x - mean
        turned = a.astype(BF16).T
        gt[g] = turned
        lt[g] = (a * d).astype(BF16).T
        ks[pl.ds(8 * g, 8), :] = jnp.dot(
            jnp.where(mine, e, 0.0).astype(BF16), turned, preferred_element_type=F32
        )

    def own_eight(j, carry):
        for i in range(8):
            center(own, de, own_at + 8 * j + i, own_to + 8 * j + i)
        return carry

    def end_eight(j, carry):
        for i in range(8):
            center(ends, dn, end_at + 8 * j + i, end_to + 8 * j + i)
        return carry

    lax.fori_loop(0, (gt.shape[0] - n_end) // 8, own_eight, 0)
    lax.fori_loop(0, n_end // 8, end_eight, 0)
    eye = lax.broadcasted_iota(jnp.int32, (128, 128), 0) == lane_id(128)

    def gather(t):
        lhs, rhs, cross = [], [], None
        for n in range(5):
            if n == 0:
                loc, tap = t + reach, None
            else:
                gap = nbr[t, n - 1] - (first + t)
                gap = jnp.where(gap < 0, gap + total, gap)
                gap = jnp.where(gap > total // 2, gap - total, gap)
                loc = t + reach + gap
                tap = 1.0 - jnp.abs(gap).astype(F32) * (1.0 / (reach + 1.0))
            g = loc // PACK
            at = pl.multiple_of(32 * (loc % PACK), 32)
            rhs.append(gt[g, pl.ds(at, 32), :])
            v = lt[g, pl.ds(at, 32), :]
            c = ks[pl.ds(8 * g + loc % PACK, 1), :]
            lhs.append(v if tap is None else (v.astype(F32) * tap).astype(BF16))
            cross = c if n == 0 else cross + tap * c
        cat = lambda v: jnp.concatenate(v, axis=0)
        dims = (((0,), (0,)), ((), ()))
        gram = lax.dot_general(cat(lhs), cat(rhs), dims, preferred_element_type=F32)
        return gram, cross

    def prepare(t):
        gram, cross = gather(t)
        total_sq = lambda a: jnp.sum(jnp.sum(a, axis=0, keepdims=True), axis=1, keepdims=True)
        diag = jnp.where(eye, gram, 0.0)
        system = gram + jnp.where(eye, 127.0, 0.0)
        inv = lax.rsqrt(total_sq(system * system))
        mid = 127.0 + total_sq(diag) * (1.0 / 128.0)
        rest = (system - jnp.where(eye, mid, 0.0)) * inv
        wide = lambda v: jnp.broadcast_to(v, (1, 128))
        return rest, wide(mid * inv), wide(inv), cross

    unit = jnp.where(eye, 1.0, 0.0)
    unit = narrow(jnp.concatenate([unit, unit], axis=1))

    def tiles(b, carry):
        ts = [b * UNROLL + u for u in range(UNROLL)]
        ready = [prepare(t) for t in ts]
        pairs = range(UNROLL // 2)
        wide = lambda j: [
            jnp.concatenate([ready[2 * p][j], ready[2 * p + 1][j]], axis=1) for p in pairs
        ]
        v, al = wide(0), wide(1)
        root = rho = None
        for step in range(3):
            vs = each(narrow, v)
            sq = each(pair_dot, vs, vs)
            be = each(lambda a: a * (0.0625 * a - 0.5625), al)
            cx = each(lambda a, c: 1.6875 + c + 0.0625 * a * a, al, be)
            c1 = each(lambda a, c: 2.0 * a * c - 2.4375 - 0.5625 * a * a, al, cx)
            ga = each(lambda a, c: 2.25 + a * (1.6875 * a - 2.4375) + a * a * c, al, be)
            xs, ys, lin = [], [], []
            for m, p, a, i, j in zip(v, sq, al, c1, cx):
                n = narrow(m)
                x = narrow(2.0 * a) * n + narrow(p)
                xs.append(x)
                ys.append(0.0625 * x - 0.5625 * n)
                lin.append(i * m + j * p)
            high = each(pair_dot, xs, ys)
            q = each(lambda m, h: m + h, lin, high)
            qs = each(narrow, q)

            def times(m, a):
                prod = each(lambda i, c, r: pair_dot(narrow(i) + unit * narrow(c), r), m, a, qs)
                rest = each(lambda g, j, d: g * j + d, ga, m, prod)
                return rest, each(lambda i, g: i * g, a, ga)

            root, rho = (q, ga) if root is None else times(root, rho)
            if step < 2:
                v, al = times(*times(v, al))
        for u, t in enumerate(ts):
            _, _, inv, cross = ready[u]
            at = 128 * (u % 2)
            r = root[u // 2][:, at : at + 128]
            r = r + jnp.where(eye, rho[u // 2][:, at : at + 128], 0.0)
            col = jnp.sum(r * cross, axis=1, keepdims=True)
            row = jnp.sum(r * col, axis=0, keepdims=True) * inv
            out[t] = (r * jnp.sqrt(127.0 * inv) + row).astype(BF16)
        return carry

    lax.fori_loop(0, out.shape[0] // UNROLL, tiles, 0)


def update_kernel(info, tr, keep, given, s1, s2, s3, *outs):
    n = tr.shape[0]

    def tile(t, carry):
        parts = [keep[t], s1[t], s2[t], s3[t], given[t], s1[n + t], s2[n + t], s3[n + t]]
        x = jnp.concatenate(parts, axis=0).astype(F32)
        mean = jnp.sum(x, axis=0, keepdims=True) * (1.0 / 128.0)
        anomaly = (x - mean).astype(BF16)
        new = jnp.dot(tr[t], anomaly, preferred_element_type=F32) + mean
        new = new.astype(BF16)
        for i, o in enumerate(outs):
            o[t] = new[16 * i : 16 * i + 16]
        return carry

    lax.fori_loop(0, n, tile, 0, unroll=8)


def place_kernel(info, *refs):
    pieces, out, buf = refs[:8], refs[8], refs[9]
    z, k = info[0], info[1]
    for i, piece in enumerate(pieces):
        d, o = i % 4, i // 4
        zz = (z + d) % 4
        kk = k if o == 0 else 1 - k
        at = pl.multiple_of(64 * zz + 32 * kk, 32)
        for t in range(32):
            buf[i % 2, pl.ds(t, 16, stride=33), :] = piece[t].astype(F32)
        for m in range(16):
            out[m, pl.ds(at, 32), :] = buf[i % 2, 33 * m : 33 * m + 32, :].astype(BF16)


def vmem():
    return pl.BlockSpec(memory_space=pltpu.VMEM)


def smem():
    return pl.BlockSpec(memory_space=pltpu.SMEM)


def call(kernel, n_smem, args, outs, scratch=(), mib=12, specs=None):
    return pl.pallas_call(
        kernel,
        in_specs=[smem()] * n_smem + list(specs or [vmem()] * (len(args) - n_smem)),
        out_specs=jax.tree.map(lambda _: vmem(), outs),
        out_shape=outs,
        scratch_shapes=list(scratch),
        compiler_params=pltpu.CompilerParams(vmem_limit_bytes=mib * 1024 * 1024),
    )(*args)


def to_z(x, by):
    return lax.ppermute(x, "z", [(i, (i + by) % 4) for i in range(4)])


def to_core(x):
    return lax.ppermute(x, "k", [(0, 1), (1, 0)])


def to_cells(x, by):
    n = lax.axis_size("cells")
    return lax.ppermute(x, "cells", [(i, (i + by) % n) for i in range(n)])


def to_side(x, d):
    n = lax.axis_size("cells")
    pairs = []
    for c in range(n):
        for z in range(4):
            zz = (z + d) % 4
            cc = (c + 1) % n if zz < 2 else (c - 1) % n
            pairs += [(8 * c + 2 * z + k, 8 * cc + 2 * zz + k) for k in range(2)]
    return lax.ppermute(x, ("cells", "z", "k"), pairs)


def home(x, d, o):
    pairs = [(2 * z + k, 2 * ((z - d) % 4) + (k ^ o)) for z in range(4) for k in range(2)]
    return lax.ppermute(x, MEM, pairs)


def analysis(bg, figures, spread, pixel, active, nbr):
    members, tiles, width = bg.shape
    groups = tiles // PACK
    z, k = lax.axis_index("z"), lax.axis_index("k")
    first = lax.axis_index("cells") * tiles + 64 * z + 32 * k
    info = jnp.stack([z, k, first, tiles * lax.axis_size("cells")]).astype(jnp.int32)
    half = groups // 2
    shape = lambda n: jax.ShapeDtypeStruct((n, members, width), BF16)
    sg, *rest = call(
        sense_kernel,
        1,
        (info, bg),
        (shape(groups),) + (shape(tiles // 8),) * 4 + (shape(tiles // 2),),
        [pltpu.VMEM((members * (tiles + 1) + 7, width), F32)],
    )
    left = to_cells(sg[half:], 1)
    right = to_cells(sg[:half], -1)
    keep, give = rest[:4], rest[4]
    given = to_core(give)
    ends = list(call(pick_kernel, 1, (info, left, right), (shape(half),) * 4))
    own = [sg] + [to_z(sg, d) for d in (1, 2, 3)]
    for d in (1, 2, 3):
        ends[d] = to_z(ends[d], d)
    both = call(both_kernel, 0, (*keep[1:], given), (shape(tiles // 4),) * 3)
    state = [to_z(both[d - 1], d) for d in (1, 2, 3)]
    de, near, own_nbr = call(
        cell_kernel,
        1,
        (info, pixel, spread, figures, active.reshape(2, tiles // 2), nbr),
        (
            jax.ShapeDtypeStruct((2, groups, 128), F32),
            jax.ShapeDtypeStruct((2, half, 128), F32),
            jax.ShapeDtypeStruct((32, 4), jnp.int32),
        ),
        [pltpu.VMEM((tiles, 128), F32)],
    )
    dn = to_side(near, 0)
    own += [to_core(r) for r in own]
    ends += [to_core(r) for r in ends]
    transform = call(
        solve_kernel,
        2,
        (info, own_nbr, *own, *ends, de, dn),
        jax.ShapeDtypeStruct((32, 128, 128), BF16),
        [
            pltpu.VMEM((72, 128, 128), BF16),
            pltpu.VMEM((72, 128, 128), BF16),
            pltpu.VMEM((8 * 72, 128), F32),
        ],
        40,
    )
    outs = call(update_kernel, 1, (info, transform, keep[0], given, *state), (shape(32),) * 8)
    back = [
        outs[i] if i == 0 else home(outs[i], i % 4, i // 4) for i in range(8)
    ]
    return call(
        place_kernel,
        1,
        (info, *back),
        jax.ShapeDtypeStruct((members, tiles, width), BF16),
        [pltpu.VMEM((2, 16 * 33, 128), F32)],
    )


def solution(mesh):
    finer = Mesh(mesh.devices.reshape(mesh.shape["cells"], 4, 2), ("cells", "z", "k"))
    placed = (
        P(MEM, "cells", None),
        P("cells", None),
        P("cells", None),
        P("cells", None),
        P("cells"),
        P("cells", None),
    )
    return jax.shard_map(
        analysis, mesh=finer, in_specs=placed, out_specs=P(MEM, "cells", None), check_vma=False
    )
```

```python
import jax
import jax.numpy as jnp
from jax import lax
from jax.experimental import pallas as pl
from jax.experimental.pallas import tpu as pltpu
from jax.sharding import Mesh
from jax.sharding import PartitionSpec as P

F32 = jnp.float32
BF16 = jnp.bfloat16
MEM = ("z", "k")
PACK = 4
UNROLL = 16


def lane_id(rows):
    return lax.broadcasted_iota(jnp.int32, (rows, 128), 1)


def sense_kernel(info, bg, sg, *refs):
    keeps, (give,), cores, buf = refs[:4], refs[4:5], refs[5:9], refs[9]
    members, tiles, _ = bg.shape
    z, k = info[0], info[1]
    pitch = tiles + 1
    row = lax.broadcasted_iota(jnp.int32, (128 * PACK, 128), 0)
    lane, q = row & 127, row >> 7
    goal = lane_id(128 * PACK) - 32 * q
    pick = jnp.where((lane == goal) & (lane < 32), 1.0, 0.0)
    pick = pick + jnp.where((lane - 32 == goal) & (lane >= 32) & (lane < 64), 0.5, 0.0)
    pick = pick.astype(BF16)
    for m in range(members):
        buf[pl.ds(m * pitch, tiles), :] = bg[m].astype(F32)
    chunk = tiles // 8
    for n in range(8):
        zone = 2 * ((z + n) % 4) + (k if n < 4 else 1 - k)
        xd, skip = (keeps[n], 0) if n < 4 else (give, chunk * (n - 4))
        rows = []
        for i in range(chunk // PACK):
            group = []
            for q in range(PACK):
                at = chunk * zone + PACK * i + q
                x = buf[pl.ds(at, members, stride=pitch), :].astype(BF16)
                xd[skip + PACK * i + q] = x
                group.append(x)
            rows.append(jnp.concatenate(group, axis=1))
        sensed = jnp.dot(jnp.concatenate(rows, axis=0), pick, preferred_element_type=F32)
        sensed = sensed.astype(BF16)
        for i in range(chunk // PACK):
            sg[(chunk // PACK) * zone + i] = sensed[members * i : members * (i + 1)]
    for d, core in enumerate(cores):
        at = jnp.where((z + d) % 4 < 2, 0, 16)
        for i in range(core.shape[0]):
            core[i] = sg[at + i]


def both_kernel(k1, k2, k3, given, *outs):
    for d, (keep, both) in enumerate(zip((k1, k2, k3), outs), 1):
        n = keep.shape[0]
        for i in range(n):
            both[i] = keep[i]
            both[n + i] = given[n * d + i]


def pick_kernel(info, sg, left, right, *outs):
    for d, end in enumerate(outs):
        zz = (info[0] + d) % 4
        for to, pieces in enumerate(
            (
                ((left, 0), (left, 16)),
                ((left, 16), (sg, 48)),
                ((sg, 0), (right, 0)),
                ((right, 0), (right, 16)),
            )
        ):

            @pl.when(zz == to)
            def _(pieces=pieces, end=end):
                for h, (ref, at) in enumerate(pieces):
                    for i in range(16):
                        end[16 * h + i] = ref[at + i]


def cell_kernel(info, pix, spread, y, active, nbr, out, near, own_nbr, w2):
    groups = pix.shape[0] // PACK
    half = pix.shape[0] // 2
    counts = jnp.concatenate([active[...]] * 4, axis=0).astype(F32).T
    slot = lane_id(half).astype(F32)
    for h in range(2):
        rows = pl.ds(half * h, half)
        w2[rows, :] = jnp.where(slot < counts[:, h : h + 1], 1.0 / spread[rows, :], 0.0)

    def packed(ref, p):
        parts = [ref[pl.ds(2 * p + h, groups, stride=PACK), :] for h in range(2)]
        return jnp.concatenate(parts, axis=0).astype(F32).T

    cols = [[], []]
    for p in range(2):
        pt = packed(pix, p)
        wt = packed(w2, p)
        yt = packed(y, p) * wt
        d, e = [], []
        for c in range(32):
            hit = pt == float(c)
            d.append(jnp.sum(jnp.where(hit, wt, 0.0), axis=0, keepdims=True))
            e.append(jnp.sum(jnp.where(hit, yt, 0.0), axis=0, keepdims=True))
        for i, rows in enumerate((d, e)):
            block = jnp.concatenate(rows, axis=0)
            cols[i] += [block, pltpu.roll(block, 64, 1)]
    at = pl.multiple_of(jnp.where(info[0] < 2, 32, 0), 32)
    for i in range(2):
        out[i] = jnp.concatenate(cols[i], axis=0).T[:groups]
        near[i] = out[i, pl.ds(at, 32), :]
    own_nbr[...] = nbr[pl.ds(pl.multiple_of(64 * info[0] + 32 * info[1], 32), 32), :]


def pair_dot(left, right):
    zero = jnp.zeros((128, 128), BF16)
    top = jnp.concatenate([right[:, :128], zero], axis=1)
    low = jnp.concatenate([zero, right[:, 128:]], axis=1)
    both = jnp.concatenate([top, low], axis=0)
    return jnp.dot(left, both, preferred_element_type=F32)


def each(f, *lists):
    return [f(*a) for a in zip(*lists)]


def narrow(a):
    return a.astype(BF16)


def solve_kernel(info, nbr, *refs):
    own, ends, (de, dn, out, gt, lt, ks, tab) = refs[:8], refs[8:16], refs[16:]
    z, k, first, total = info[0], info[1], info[2], info[3]
    reach = 128
    for i in range(2):
        tab[i, 32:96, :] = de[i]
        tab[i, pl.ds(pl.multiple_of(jnp.where(z < 2, 0, 96), 32), 32), :] = dn[i]
    lead = jnp.where(z == 0, 32, jnp.where(z == 3, 0, 16))
    here = 8 * k
    own_lo = jnp.maximum(lead, here)
    own_hi = jnp.minimum(lead + 48, here + 72)
    n_first = (own_lo - here) // 8
    n_last = (here + 72 - own_hi) // 8
    mine = lax.broadcasted_iota(jnp.int32, (8, 128), 0) == (lane_id(8) >> 5)

    def center(src, b, w):
        g = w - here
        x = jnp.concatenate([r[b] for r in src], axis=0).astype(F32)
        mean = jnp.sum(x, axis=0, keepdims=True) * (1.0 / 128.0)
        d = tab[0, pl.ds(16 * z + w, 1), :]
        e = tab[1, pl.ds(16 * z + w, 1), :] - d * mean
        a = x - mean
        turned = a.astype(BF16).T
        gt[g] = turned
        lt[g] = (a * d).astype(BF16).T
        ks[pl.ds(8 * g, 8), :] = jnp.dot(
            jnp.where(mine, e, 0.0).astype(BF16), turned, preferred_element_type=F32
        )

    def own_eight(j, carry):
        for i in range(8):
            w = own_lo + 8 * j + i
            center(own, w - lead, w)
        return carry

    def end_eight(j, carry):
        early = j < n_first
        w0 = jnp.where(early, here + 8 * j, own_hi + 8 * (j - n_first))
        b0 = jnp.where(early, w0, w0 - 48)
        for i in range(8):
            center(ends, b0 + i, w0 + i)
        return carry

    lax.fori_loop(0, (own_hi - own_lo) // 8, own_eight, 0)
    lax.fori_loop(0, n_first + n_last, end_eight, 0)
    eye = lax.broadcasted_iota(jnp.int32, (128, 128), 0) == lane_id(128)

    def gather(t):
        lhs, rhs, cross = [], [], None
        for n in range(5):
            if n == 0:
                loc, tap = t + reach, None
            else:
                gap = nbr[t, n - 1] - (first + t)
                gap = jnp.where(gap < 0, gap + total, gap)
                gap = jnp.where(gap > total // 2, gap - total, gap)
                loc = t + reach + gap
                tap = 1.0 - jnp.abs(gap).astype(F32) * (1.0 / (reach + 1.0))
            g = loc // PACK
            at = pl.multiple_of(32 * (loc % PACK), 32)
            rhs.append(gt[g, pl.ds(at, 32), :])
            v = lt[g, pl.ds(at, 32), :]
            c = ks[pl.ds(8 * g + loc % PACK, 1), :]
            lhs.append(v if tap is None else (v.astype(F32) * tap).astype(BF16))
            cross = c if n == 0 else cross + tap * c
        cat = lambda v: jnp.concatenate(v, axis=0)
        dims = (((0,), (0,)), ((), ()))
        gram = lax.dot_general(cat(lhs), cat(rhs), dims, preferred_element_type=F32)
        return gram, cross

    def prepare(t):
        gram, cross = gather(t)
        total_sq = lambda a: jnp.sum(jnp.sum(a, axis=0, keepdims=True), axis=1, keepdims=True)
        diag = jnp.where(eye, gram, 0.0)
        system = gram + jnp.where(eye, 127.0, 0.0)
        inv = lax.rsqrt(total_sq(system * system))
        mid = 127.0 + total_sq(diag) * (1.0 / 128.0)
        rest = (system - jnp.where(eye, mid, 0.0)) * inv
        wide = lambda v: jnp.broadcast_to(v, (1, 128))
        return rest, wide(mid * inv), wide(inv), cross

    unit = jnp.where(eye, 1.0, 0.0)
    unit = narrow(jnp.concatenate([unit, unit], axis=1))

    def tiles(b, carry):
        ts = [b * UNROLL + u for u in range(UNROLL)]
        ready = [prepare(t) for t in ts]
        pairs = range(UNROLL // 2)
        wide = lambda j: [
            jnp.concatenate([ready[2 * p][j], ready[2 * p + 1][j]], axis=1) for p in pairs
        ]
        v, al = wide(0), wide(1)
        root = rho = None
        for step in range(3):
            vs = each(narrow, v)
            sq = each(pair_dot, vs, vs)
            be = each(lambda a: a * (0.0625 * a - 0.5625), al)
            cx = each(lambda a, c: 1.6875 + c + 0.0625 * a * a, al, be)
            c1 = each(lambda a, c: 2.0 * a * c - 2.4375 - 0.5625 * a * a, al, cx)
            ga = each(lambda a, c: 2.25 + a * (1.6875 * a - 2.4375) + a * a * c, al, be)
            xs, ys, lin = [], [], []
            for m, p, a, i, j in zip(v, sq, al, c1, cx):
                n = narrow(m)
                x = narrow(2.0 * a) * n + narrow(p)
                xs.append(x)
                ys.append(0.0625 * x - 0.5625 * n)
                lin.append(i * m + j * p)
            high = each(pair_dot, xs, ys)
            q = each(lambda m, h: m + h, lin, high)
            qs = each(narrow, q)

            def times(m, a):
                prod = each(lambda i, c, r: pair_dot(narrow(i) + unit * narrow(c), r), m, a, qs)
                rest = each(lambda g, j, d: g * j + d, ga, m, prod)
                return rest, each(lambda i, g: i * g, a, ga)

            root, rho = (q, ga) if root is None else times(root, rho)
            if step < 2:
                v, al = times(*times(v, al))
        for u, t in enumerate(ts):
            _, _, inv, cross = ready[u]
            at = 128 * (u % 2)
            r = root[u // 2][:, at : at + 128]
            r = r + jnp.where(eye, rho[u // 2][:, at : at + 128], 0.0)
            col = jnp.sum(r * cross, axis=1, keepdims=True)
            row = jnp.sum(r * col, axis=0, keepdims=True) * inv
            out[t] = (r * jnp.sqrt(127.0 * inv) + row).astype(BF16)
        return carry

    lax.fori_loop(0, out.shape[0] // UNROLL, tiles, 0)


def update_kernel(info, tr, keep, given, s1, s2, s3, *outs):
    n = tr.shape[0]

    def tile(t, carry):
        parts = [keep[t], s1[t], s2[t], s3[t], given[t], s1[n + t], s2[n + t], s3[n + t]]
        x = jnp.concatenate(parts, axis=0).astype(F32)
        mean = jnp.sum(x, axis=0, keepdims=True) * (1.0 / 128.0)
        anomaly = (x - mean).astype(BF16)
        new = jnp.dot(tr[t], anomaly, preferred_element_type=F32) + mean
        new = new.astype(BF16)
        for i, o in enumerate(outs):
            o[t] = new[16 * i : 16 * i + 16]
        return carry

    lax.fori_loop(0, n, tile, 0, unroll=8)


def place_kernel(info, *refs):
    pieces, out, buf = refs[:8], refs[8], refs[9]
    z, k = info[0], info[1]
    for i, piece in enumerate(pieces):
        d, o = i % 4, i // 4
        zz = (z + d) % 4
        kk = k if o == 0 else 1 - k
        at = pl.multiple_of(64 * zz + 32 * kk, 32)
        for t in range(32):
            buf[i % 2, pl.ds(t, 16, stride=33), :] = piece[t].astype(F32)
        for m in range(16):
            out[m, pl.ds(at, 32), :] = buf[i % 2, 33 * m : 33 * m + 32, :].astype(BF16)


def vmem():
    return pl.BlockSpec(memory_space=pltpu.VMEM)


def smem():
    return pl.BlockSpec(memory_space=pltpu.SMEM)


def call(kernel, n_smem, args, outs, scratch=(), mib=12, specs=None):
    return pl.pallas_call(
        kernel,
        in_specs=[smem()] * n_smem + list(specs or [vmem()] * (len(args) - n_smem)),
        out_specs=jax.tree.map(lambda _: vmem(), outs),
        out_shape=outs,
        scratch_shapes=list(scratch),
        compiler_params=pltpu.CompilerParams(vmem_limit_bytes=mib * 1024 * 1024),
    )(*args)


def to_z(x, by):
    return lax.ppermute(x, "z", [(i, (i + by) % 4) for i in range(4)])


def to_core(x):
    return lax.ppermute(x, "k", [(0, 1), (1, 0)])


def to_cells(x, by):
    n = lax.axis_size("cells")
    return lax.ppermute(x, "cells", [(i, (i + by) % n) for i in range(n)])


def to_side(x, d):
    n = lax.axis_size("cells")
    pairs = []
    for c in range(n):
        for z in range(4):
            zz = (z + d) % 4
            cc = (c + 1) % n if zz < 2 else (c - 1) % n
            pairs += [(8 * c + 2 * z + k, 8 * cc + 2 * zz + k) for k in range(2)]
    return lax.ppermute(x, ("cells", "z", "k"), pairs)


def home(x, d, o):
    pairs = [(2 * z + k, 2 * ((z - d) % 4) + (k ^ o)) for z in range(4) for k in range(2)]
    return lax.ppermute(x, MEM, pairs)


def analysis(bg, figures, spread, pixel, active, nbr):
    members, tiles, width = bg.shape
    groups = tiles // PACK
    z, k = lax.axis_index("z"), lax.axis_index("k")
    first = lax.axis_index("cells") * tiles + 64 * z + 32 * k
    info = jnp.stack([z, k, first, tiles * lax.axis_size("cells")]).astype(jnp.int32)
    half = groups // 2
    shape = lambda n: jax.ShapeDtypeStruct((n, members, width), BF16)
    sg, *rest = call(
        sense_kernel,
        1,
        (info, bg),
        (shape(groups),) + (shape(tiles // 8),) * 4 + (shape(tiles // 2),) + (shape(48),) * 4,
        [pltpu.VMEM(((members + 1) * (tiles + 1) + 7, width), F32)],
    )
    left = to_cells(sg[half:], 1)
    right = to_cells(sg[:half], -1)
    keep, give = rest[:4], rest[4]
    given = to_core(give)
    ends = list(call(pick_kernel, 1, (info, sg, left, right), (shape(half),) * 4))
    own = [rest[5]] + [to_z(rest[5 + d], d) for d in (1, 2, 3)]
    for d in (1, 2, 3):
        ends[d] = to_z(ends[d], d)
    both = call(both_kernel, 0, (*keep[1:], given), (shape(tiles // 4),) * 3)
    state = [to_z(both[d - 1], d) for d in (1, 2, 3)]
    de, near, own_nbr = call(
        cell_kernel,
        1,
        (info, pixel, spread, figures, active.reshape(2, tiles // 2), nbr),
        (
            jax.ShapeDtypeStruct((2, groups, 128), F32),
            jax.ShapeDtypeStruct((2, half, 128), F32),
            jax.ShapeDtypeStruct((32, 4), jnp.int32),
        ),
        [pltpu.VMEM((tiles, 128), F32)],
    )
    dn = to_side(near, 0)
    own += [to_core(r) for r in own]
    ends += [to_core(r) for r in ends]
    transform = call(
        solve_kernel,
        2,
        (info, own_nbr, *own, *ends, de, dn),
        jax.ShapeDtypeStruct((32, 128, 128), BF16),
        [
            pltpu.VMEM((72, 128, 128), BF16),
            pltpu.VMEM((72, 128, 128), BF16),
            pltpu.VMEM((8 * 72, 128), F32),
            pltpu.VMEM((2, 128, 128), F32),
        ],
        40,
    )
    outs = call(update_kernel, 1, (info, transform, keep[0], given, *state), (shape(32),) * 8)
    back = [outs[i] if i == 0 else home(outs[i], i % 4, i // 4) for i in range(8)]
    return call(
        place_kernel,
        1,
        (info, *back),
        jax.ShapeDtypeStruct((members, tiles, width), BF16),
        [pltpu.VMEM((2, 17 * 33 + 7, 128), F32)],
    )


def solution(mesh):
    finer = Mesh(mesh.devices.reshape(mesh.shape["cells"], 4, 2), ("cells", "z", "k"))
    placed = (
        P(MEM, "cells", None),
        P("cells", None),
        P("cells", None),
        P("cells", None),
        P("cells"),
        P("cells", None),
    )
    return jax.shard_map(
        analysis, mesh=finer, in_specs=placed, out_specs=P(MEM, "cells", None), check_vma=False
    )
```
